256 devices in a mesh: tm: 64 (over y, z, core), space: 4 (over x).
Axes of the slice: x: 4, y: 4, z: 8, core: 2. Of those that a mesh axis runs over, the one named last changes fastest.
Arguments:
- starts: float32 [64, 5, 16, 64, 128], P('tm', None, 'space'), may hold values from -4 to 4
- source: float32 [5, 16, 64, 128], P(None, 'space'), may hold values from -4 to 4
Outputs:
- ends: float32 [64, 5, 16, 64, 128], P('tm', None, 'space')
- slice_norms: float32 [64], P('tm')
- total_norm: float32 [1], replicated
The draws below stay inside these ranges and needn't reach their ends.
All inputs are finite; a program needn't handle non-finite values.
Results may differ from the reference program's by a relative error of at most 0.0003.
Values sent between devices are 32-bit elements; how exact they have to be, the bound alone decides.
A program may use at most 64 MiB of HBM per device.

```python
import math
import jax
import jax.numpy as jnp
from jax import lax

FIELDS = 5
NX = 128
NY = 64
STEPS = 1
NZ = 16
SLICES = 64


def block_levels(rng, dims, cuts, least, top_value):
    gain, own = 1.0, jax.random.fold_in(rng, 6)
    for position, parts in cuts:
        draws = jnp.exp(jax.random.uniform(jax.random.fold_in(own, position), (parts,), jnp.float32, least / len(cuts), top_value / len(cuts)))
        gain = gain * jnp.repeat(draws, dims[position] // parts).reshape([-1 if axis == position else 1 for axis in range(len(dims))])
    return gain


def normal_values(stream_key, extent, deviation, reach, split=(), kind=jnp.bfloat16):
    entries = jax.random.normal(stream_key, extent, jnp.float32) * deviation
    if len(split) > 0:
        entries = block_levels(stream_key, extent, split, -0.22, 0.18) * entries
    return jnp.clip(entries, min=-reach, max=reach).astype(kind)


def setup_inputs(seed: int = 0) -> dict:
    key_of = jax.random.split(jax.random.key(seed), 3)
    return {
        "starts": normal_values(key_of[0], (SLICES, FIELDS, NZ, NY, NX), 0.3, 4.0, ((0, 64), (2, 4)), jnp.float32),
        "source": normal_values(key_of[1], (FIELDS, NZ, NY, NX), 0.3, 4.0, ((1, 4),), jnp.float32),
    }


viscosity = 0.08
diffusivity = 0.05
compress_rate = 0.25
time_step = 0.5
diffusion_number = 0.08
advect_xaxis = 0.2
advect_yaxis = 0.15
advect_zaxis = 0.1
epsilon = 1e-06

def central(values, axis):
    return 0.5 * (jnp.roll(values, -1, axis) - jnp.roll(values, 1, axis))

def laplace(values):
    summed = -6.0 * values
    for axis in (0, 1, 2):
        summed = summed + jnp.roll(values, -1, axis) + jnp.roll(values, 1, axis)
    return summed

def tendency(state_now, source):
    speed_xaxis = advect_xaxis + state_now[0]
    speed_yaxis = advect_yaxis + state_now[1]
    speed_zaxis = advect_zaxis + state_now[2]

    def transport(quantity):
        return central(speed_xaxis * quantity, 2) + central(speed_yaxis * quantity, 1) + central(speed_zaxis * quantity, 0)
    pressure = state_now[3]
    xmomentum = -transport(state_now[0]) - central(pressure, 2) + viscosity * laplace(state_now[0])
    ymomentum = -transport(state_now[1]) - central(pressure, 1) + viscosity * laplace(state_now[1])
    zmomentum = -transport(state_now[2]) - central(pressure, 0) + viscosity * laplace(state_now[2])
    pressure_rate = -compress_rate * (central(state_now[0], 2) + central(state_now[1], 1) + central(state_now[2], 0))
    scalar_rate = -transport(state_now[4]) + diffusivity * laplace(state_now[4])
    return jnp.stack([xmomentum, ymomentum, zmomentum, pressure_rate, scalar_rate]) + source

def fine_run(current, source):
    for repeat in range(STEPS):
        section_one = tendency(current, source)
        section_two = tendency(current + 0.5 * time_step * section_one, source)
        section_three = tendency(current + 0.5 * time_step * section_two, source)
        section_four = tendency(current + time_step * section_three, source)
        current = current + time_step / 6.0 * (section_one + 2.0 * section_two + 2.0 * section_three + section_four)
    return current

def signed_angle(length):
    cell_ids = jnp.arange(length, dtype=jnp.int32)
    signed = (cell_ids + length // 2) % length - length // 2
    return (signed, 2.0 * math.pi / length * signed.astype(jnp.float32))

def coarse_symbol():
    zsigned, zangles = signed_angle(NZ)
    ysigned, yangles = signed_angle(NY)
    xsigned, xangles = signed_angle(NX)
    keeper = ((jnp.abs(ysigned) < NY // 8)[:, None] & (jnp.abs(xsigned) < NX // 16)[None, :]).astype(jnp.float32)
    real_part = 1.0 + diffusion_number * ((2.0 * jnp.cos(zangles) - 2.0)[:, None, None] + (2.0 * jnp.cos(yangles) - 2.0)[None, :, None] + (2.0 * jnp.cos(xangles) - 2.0)[None, None, :])
    imag_part = -(advect_zaxis * jnp.sin(zangles)[:, None, None] + advect_yaxis * jnp.sin(yangles)[None, :, None] + advect_xaxis * jnp.sin(xangles)[None, None, :])
    return lax.complex(real_part * keeper[None], imag_part * keeper[None])

def coarse(values, symbol):
    spectrum = jnp.fft.fftn(values, axes=(1, 2, 3))
    return jnp.real(jnp.fft.ifftn(spectrum * symbol, axes=(1, 2, 3)))

def reference(starts, source):

    def run_slice(begin_state):
        return fine_run(begin_state, source)
    fine = lax.map(run_slice, starts)
    symbol = coarse_symbol()

    def advance(carried, inputs_pair):
        old_start, fine_end = inputs_pair
        end_state = fine_end + coarse(carried - old_start, symbol)
        jump_size = end_state - fine_end
        return (end_state, (end_state, jnp.sum(jump_size * jump_size)))
    unused, (ends, sums) = lax.scan(advance, starts[0], (starts, fine))
    cell_total = FIELDS * NZ * NY * NX
    slice_norms = jnp.sqrt(sums / cell_total + epsilon)
    total_norm = jnp.sqrt(jnp.sum(sums) / (cell_total * SLICES) + epsilon).reshape(1)
    return (ends, slice_norms, total_norm)
```

```python
import functools
import math

import jax
import jax.numpy as jnp
import numpy as np
from jax import lax
from jax.experimental import pallas as pl
from jax.experimental.pallas import tpu as pltpu
from jax.sharding import Mesh
from jax.sharding import PartitionSpec as P

Y, Z, C, X = "tm_0", "tm_1", "tm_2", "space"
TM = (Y, Z, C)
MESH = pl.DeviceIdType.MESH
F32, BF16 = jnp.float32, jnp.bfloat16

FIELDS, NZ, NY, NX, SLICES = 5, 16, 64, 128, 64
SLABS, DEPTH = 4, 4
KX, KY = NX // 16, NY // 8
CELLS = NZ * NY * NX
viscosity, diffusivity, compress_rate = 0.08, 0.05, 0.25
time_step, diffusion_number = 0.5, 0.08
advect = {"x": 0.2, "y": 0.15, "z": 0.1}
epsilon = 1e-06
GREETINGS = (None, 2, 6, 10, 14, 18, 22, 26)
PASS_ON = 18
QUARTERS = 4
ROWS = FIELDS * KX
Q_LANE, T_LANE = 64, 72


def halves(table):
    table = np.asarray(table, np.float32)
    high = table.astype(BF16)
    low = (table - high.astype(np.float32)).astype(BF16)
    return high, low


def tables():
    kx, xs = np.arange(KX), np.arange(NX)
    ky = (np.arange(2 * KY) + KY) % (2 * KY) - KY
    keep = (ky != -KY).astype(np.float64)
    ax = 2 * np.pi / NX * np.outer(kx, xs)
    cx = np.concatenate([np.cos(ax), np.sin(ax)])
    weight = np.where(kx == 0, 1.0, 2.0)[:, None]
    cinv = np.concatenate([weight * np.cos(ax), weight * np.sin(ax)])
    permuted = np.arange(NY).reshape(8, 8).T.reshape(-1)
    eye = np.eye(DEPTH)

    def plane(ys):
        ay = 2 * np.pi / NY * np.outer(ys, ky)
        return np.cos(ay) * keep, np.sin(ay) * keep

    co, si = plane(permuted)
    m1 = np.zeros((2, DEPTH, NY, DEPTH, 2, 2 * KY))
    for cs, (re, im) in enumerate(((co, -si), (-si, -co))):
        m1[cs, :, :, :, 0, :] = np.einsum("ab,yk->aybk", eye, re)
        m1[cs, :, :, :, 1, :] = np.einsum("ab,yk->aybk", eye, im)
    co, si = plane(np.arange(NY))
    m4 = np.zeros((DEPTH, 2, 2 * KY, 2, DEPTH, NY))
    for cs, (re, im) in enumerate(((co, -si), (-si, -co))):
        m4[:, 0, :, cs, :, :] = np.einsum("ab,yk->akby", eye, re) / CELLS
        m4[:, 1, :, cs, :, :] = np.einsum("ab,yk->akby", eye, im) / CELLS
    m1 = m1.reshape(512, DEPTH, 2, QUARTERS, 4).transpose(0, 3, 1, 2, 4)
    m4 = m4.reshape(DEPTH, 2, QUARTERS, 4, 512).transpose(2, 0, 1, 3, 4)
    zs, kz = np.arange(NZ), np.arange(NZ)
    az = 2 * np.pi / NZ * np.outer(zs, kz)
    same = np.eye(2 * KY) * keep
    m2 = np.zeros((NZ, 2, 2 * KY, 2, NZ, 2 * KY))
    m3 = np.zeros((2, NZ, 2 * KY, NZ, 2, 2 * KY))
    for i, o, fwd in ((0, 0, np.cos(az)), (0, 1, -np.sin(az)), (1, 0, np.sin(az)), (1, 1, np.cos(az))):
        m2[:, i, :, o, :, :] = np.einsum("zq,kl->zkql", fwd, same)
        m3[o, :, :, :, i, :] = np.einsum("zq,kl->qkzl", fwd, same)
    kzs = (kz + NZ // 2) % NZ - NZ // 2
    tz, ty = 2 * np.pi / NZ * kzs, 2 * np.pi / NY * ky
    tx = 2 * np.pi / NX * kx
    real = 1.0 + diffusion_number * (
        (2 * np.cos(tz) - 2)[None, :, None] + (2 * np.cos(ty) - 2)[None, None, :] + (2 * np.cos(tx) - 2)[:, None, None]
    )
    imag = -(
        advect["z"] * np.sin(tz)[None, :, None] + advect["y"] * np.sin(ty)[None, None, :] + advect["x"] * np.sin(tx)[:, None, None]
    )
    g = ((real + 1j * imag) * keep).reshape(KX, NZ * 2 * KY)
    powers = np.zeros((KX, 8, 2 * NZ * 2 * KY))
    for p in range(6):
        power = g ** (2**p)
        powers[:, p] = np.concatenate([power.real, power.imag], axis=1)
    m2 = m2.reshape(SLABS, DEPTH, 2, QUARTERS, 4, 512).transpose(0, 3, 1, 2, 4, 5)
    m3 = m3.reshape(512, SLABS, DEPTH, 2, QUARTERS, 4).transpose(0, 1, 4, 2, 3, 5)
    return dict(
        cx=np.concatenate(halves(cx)),
        m1=np.stack(halves(m1.reshape(512, 128))),
        m2=np.stack(halves(m2.reshape(512, 512))),
        m3=np.stack(halves(m3.reshape(512, 512))),
        powers=powers.astype(np.float32),
        m4=np.stack(halves(m4.reshape(128, 512))),
        cinv=np.concatenate([halves(cinv)[0], halves(cinv)[0], halves(cinv)[1]]),
    )


def split(x):
    high = x.astype(BF16)
    return high, (x - high.astype(F32)).astype(BF16)


def dot(a, b, dims=((1,), (0,))):
    return lax.dot_general(a, b, (dims, ((), ())), preferred_element_type=F32)


def product(x, high, low):
    m = x.shape[0]
    xh, xl = split(x)
    both = dot(jnp.concatenate([xh, xl], axis=0), high)
    return both[:m] + both[m:] + dot(xh, low)


def low_modes(field_rows, cx, m1):
    out = []
    for f in range(FIELDS):
        high, low = split(field_rows(f))
        a = dot(cx, high, ((1,), (1,)))
        a = a[:16] + a[16:] + dot(cx[:16], low, ((1,), (1,)))
        out.append(jnp.concatenate([a[:KX], a[KX:]], axis=1))
    return product(jnp.concatenate(out, axis=0), m1[0], m1[1])


def rem(a, n):
    return lax.rem(a, jnp.int32(n))


def picked(i, values):
    out = jnp.int32(values[-1])
    for k, v in enumerate(values[:-1]):
        out = jnp.where(i == k, jnp.int32(v), out)
    return out


def main_kernel(
    starts, source, cx_h, m1_h, m2_h, m3_h, pw_h,
    fine_out, back_out,
    st, sr, q, halo, fo, fn, cx, m1, m2, m3, pw,
    spec_s, after, spec_f, got, turn, back,
    in_sem, const_sem, out_sem, hs, hr, rounds, p_send, p_recv, f_send, f_recv, c_send, c_recv,
):
    x, y, z, c = (lax.axis_index(a) for a in (X, Y, Z, C))
    at = lambda x=x, y=y, z=z, c=c: {Y: y, Z: z, C: c, X: x}
    up, down = at(x=rem(x + 1, 4)), at(x=rem(x + 3, 4))
    load_s = [
        pltpu.make_async_copy(starts.at[0, :, pl.ds(p, n)], st.at[:, pl.ds(p, n)], in_sem.at[i])
        for i, (p, n) in ((0, (0, 1)), (0, (3, 1)), (1, (1, 2)))
    ]
    load_r = pltpu.make_async_copy(source, sr, in_sem.at[2])
    for copy in load_s[:2]:
        copy.start()
    consts = [
        pltpu.make_async_copy(a, b, const_sem.at[i])
        for i, (a, b) in ((0, (cx_h, cx)), (0, (m1_h, m1)), (1, (m2_h, m2)), (1, (m3_h, m3)))
    ]
    scan_x2z = x * 2 + rem(z, 2)
    load_p = pltpu.make_async_copy(pw_h.at[scan_x2z], pw, const_sem.at[1])

    barrier = pltpu.get_barrier_semaphore()
    around = [
        up, down, at(y=rem(y + 1, 4)), at(y=rem(y + 3, 4)), at(z=rem(z + 1, 8)), at(z=rem(z + 7, 8)), at(c=1 - c),
    ]
    for device in around:
        pl.semaphore_signal(barrier, inc=1, device_id=device, device_id_type=MESH)

    def greet(k):
        for turn_by in (1, -1):
            device = (
                at(x=rem(x + turn_by + 4, 4)), at(c=1 - c),
                at(y=rem(y + turn_by + 4, 4)), at(y=rem(y + turn_by + 4, 4)),
                *[at(z=rem(z + turn_by + 8, 8))] * 4,
            )[k]
            pl.semaphore_signal(rounds.at[k], inc=1, device_id=device, device_id_type=MESH)

    load_s[0].wait()
    load_s[1].wait()
    load_s[2].start()

    def lay(planes):
        def body(r, carry):
            for plane in planes:
                for f in range(FIELDS):
                    q[0, r + 1, plane, f] = st[f, plane, pl.ds(r, 8, stride=8), :]
            return carry
        lax.fori_loop(0, 8, body, 0)

    def edges(j, last):
        for plane in range(DEPTH):
            for f in range(FIELDS):
                if last:
                    q[j, 0, plane, f] = pltpu.roll(q[j, 8, plane, f], 1, 0)
                else:
                    q[j, 9, plane, f] = pltpu.roll(q[j, 1, plane, f], 7, 0)

    def sends(j, r):
        return (
            pltpu.make_async_remote_copy(
                q.at[j, r + 1, 0], halo.at[j, 1, r], hs, hr.at[j % 2, r], device_id=down, device_id_type=MESH
            ),
            pltpu.make_async_remote_copy(
                q.at[j, r + 1, DEPTH - 1], halo.at[j, 0, r], hs, hr.at[j % 2, r], device_id=up, device_id_type=MESH
            ),
        )

    lay((0, 3))
    pl.semaphore_wait(barrier, len(around))
    greet(0)

    def first(r, carry):
        for copy in sends(0, r):
            copy.start()
        return carry
    lax.fori_loop(0, 8, first, 0)
    for copy in (*consts[:2], load_r, *consts[2:], load_p):
        copy.start()
    load_s[2].wait()
    lay((1, 2))
    edges(0, False)
    edges(0, True)

    consts[0].wait()
    consts[1].wait()
    spec_s[...] = low_modes(
        lambda f: jnp.concatenate([q[0, 1:9, p, f].reshape(NY, NX) for p in range(DEPTH)], axis=0), cx[...], m1
    )
    load_r.wait()

    is_owner = c == 1
    has_two = is_owner & (y == rem(scan_x2z, 4))
    mine = (y * 8 + z) * 2 + c

    before = rem(mine + SLICES - 1, SLICES)
    pass_on = pltpu.make_async_remote_copy(
        spec_s, after, p_send, p_recv,
        device_id=at(y=lax.div(before, jnp.int32(16)), z=rem(lax.div(before, jnp.int32(2)), 8), c=rem(before, 2)),
        device_id_type=MESH,
    )

    def spread(tz):
        slot = x * SLICES + rem(mine + 1, SLICES)
        for dx in (2, 1, 3, 0):
            tx = rem(x + dx, 4)
            kx = tx * 2 + rem(tz, 2)
            for dy in (2, 1, 3, 0, None):
                ty = rem(kx, 4) if dy is None else rem(y + dy, 4)
                row = (32 if dy is None else ty * KX) + kx
                here = spec_f.at[pl.ds(row, 1)]
                there = got.at[pl.ds(slot + (SLABS * SLICES if dy is None else 0), 1)]

                def far():
                    pltpu.make_async_remote_copy(
                        here, there, f_send, f_recv, device_id=at(tx, ty, tz, jnp.int32(1)), device_id_type=MESH
                    ).start()

                if dx or dy:
                    far()
                    continue
                own = (tz == z) & (ty == y) & is_owner
                pl.when(jnp.logical_not(own))(far)

                @pl.when(own)
                def _():
                    pltpu.make_async_copy(here, there, f_recv).start()

    def stage(j):
        def body(i, carry):
            r = rem(i + j, 8)
            pltpu.make_async_copy(halo.at[j, :, r], halo.at[j, :, r], hr.at[j % 2, r]).wait()
            for k, turn_at in enumerate(GREETINGS):
                if turn_at is None or turn_at // 8 != j:
                    continue

                @pl.when(i == turn_at % 8)
                def _():
                    pl.semaphore_wait(rounds.at[k - 1], 2)
                    greet(k)
                    if turn_at == PASS_ON:
                        pass_on.start()

            for plane in (0, 3, 1, 2):
                cur = [q[j, r + 1, plane, f] for f in range(FIELDS)]
                yp = [q[j, r + 2, plane, f] for f in range(FIELDS)]
                ym = [q[j, r, plane, f] for f in range(FIELDS)]
                zp = [(halo[j, 1, r, f] if plane == 3 else q[j, r + 1, plane + 1, f]) for f in range(FIELDS)]
                zm = [(halo[j, 0, r, f] if plane == 0 else q[j, r + 1, plane - 1, f]) for f in range(FIELDS)]

                def flux(v, axis, sign):
                    half = 0.5 * advect["xyz"[axis]] + 0.5 * v[axis]
                    a = viscosity - half if sign > 0 else viscosity + half
                    b = diffusivity - half if sign > 0 else diffusivity + half
                    out = [a * v[0], a * v[1], a * v[2], b * v[4]]
                    push = 0.5 * v[3]
                    out[axis] = out[axis] - push if sign > 0 else out[axis] + push
                    return out

                xplus = [pltpu.roll(v, NX - 1, 1) for v in flux(cur, 0, 1)]
                xminus = [pltpu.roll(v, 1, 1) for v in flux(cur, 0, -1)]
                parts = (xplus, xminus, flux(yp, 1, 1), flux(ym, 1, -1), flux(zp, 2, 1), flux(zm, 2, -1))
                diverge = (
                    (pltpu.roll(cur[0], NX - 1, 1) - pltpu.roll(cur[0], 1, 1)) + (yp[1] - ym[1]) + (zp[2] - zm[2])
                )
                src = [sr[f, plane, pl.ds(r, 8, stride=8), :] for f in range(FIELDS)]
                rates = [None] * FIELDS
                for n, f in enumerate((0, 1, 2, 4)):
                    coefficient = -6.0 * (viscosity if f < 3 else diffusivity)
                    total = coefficient * cur[f] + src[f]
                    pairs = [p[n] for p in parts]
                    rates[f] = total + ((pairs[0] + pairs[1]) + (pairs[2] + pairs[3]) + (pairs[4] + pairs[5]))
                rates[3] = src[3] - (0.5 * compress_rate) * diverge
                for f in range(FIELDS):
                    begin = q[0, r + 1, plane, f]
                    if j < 3:
                        step = time_step * (0.5 if j < 2 else 1.0)
                        q[j + 1, r + 1, plane, f] = begin + step * rates[f]
                    else:
                        two = q[2, r + 1, plane, f]
                        states = (q[1, r + 1, plane, f] + two) + (two + cur[f]) - begin
                        fo[f, plane, pl.ds(pl.multiple_of(r * 8, 8), 8), :] = (1.0 / 3.0) * states + (
                            time_step / 6.0
                        ) * rates[f]
            if j < 3:
                for copy in sends(j + 1, r):
                    copy.start()
                pl.when(r == 0)(lambda: edges(j + 1, False))
                pl.when(r == 7)(lambda: edges(j + 1, True))
            return carry
        lax.fori_loop(0, 8, body, 0)

    for j in range(4):
        stage(j)
    pl.semaphore_wait(rounds.at[7], 2)

    modes = low_modes(lambda f: fo[f].reshape(DEPTH * NY, NX), cx[...], m1)
    pass_on.wait_recv()
    spec_f[...] = modes - after[...]

    def fine_rows(i, carry):
        spread(picked(i, (0, 1, 7, 2, 6, 3, 5, 4)))
        return carry
    lax.fori_loop(0, 8, fine_rows, 0)

    def plain(a, carry):
        for f in range(FIELDS):
            for p in range(DEPTH):
                fn[f, p, pl.ds(pl.multiple_of(a * 8, 8), 8), :] = fo[f, p, pl.ds(a, 8, stride=8), :]
        return carry
    lax.fori_loop(0, 8, plain, 0)
    store = pltpu.make_async_copy(fn, fine_out, out_sem)
    store.start()
    consts[2].wait()
    consts[3].wait()
    load_p.wait()

    def whole(ref, n, sem):
        pltpu.make_async_copy(ref.at[pl.ds(0, n)], ref.at[pl.ds(0, n)], sem).wait()

    def own(tasks):
        whole(got, tasks * SLABS * SLICES, f_recv)
        later = lax.broadcasted_iota(jnp.int32, (SLICES, 128), 0) > 0
        blocks = []
        for t in range(tasks):
            at_row = lambda s: (t * SLABS + s) * SLICES
            jumps = [jnp.where(later, got[at_row(s) : at_row(s) + SLICES], 0.0) for s in range(SLABS)]
            blocks.append(jnp.concatenate(jumps, axis=1))
        modes = product(jnp.concatenate(blocks, axis=0), m2[0], m2[1])
        half = NZ * 2 * KY

        def times(p, re, im):
            gr, gi = pw[p : p + 1, :half], pw[p : p + 1, half:]
            return gr * re - gi * im, gr * im + gi * re

        weight = jnp.where(scan_x2z == 0, 1.0, 2.0) / CELLS
        fixes, sums = [], []
        for t in range(tasks):
            one = modes[t * SLICES : (t + 1) * SLICES]
            re, im = times(0, one[:, :half], one[:, half:])
            for p in range(6):
                zero = jnp.zeros((2**p, half), F32)
                shifted = (jnp.concatenate([zero, v[: -(2**p)]], axis=0) for v in (re, im))
                pr, pi = times(p, *shifted)
                re, im = re + pr, im + pi
            sums.append(jnp.sum(re * re + im * im, axis=1, keepdims=True) * weight)
            fixes.append(jnp.concatenate([re, im], axis=1))
        out = product(jnp.concatenate(fixes, axis=0), m3[0], m3[1])
        lane = lax.broadcasted_iota(jnp.int32, (SLICES, 128), 1)
        for t in range(tasks):
            total = jnp.sum(sums[t], axis=0, keepdims=True)
            for s in range(SLABS):
                piece = out[t * SLICES : (t + 1) * SLICES, s * 128 : (s + 1) * 128]
                row = (t * SLABS + s) * SLICES
                turn[row : row + SLICES] = jnp.where(lane == T_LANE, total, jnp.where(lane == Q_LANE, sums[t], piece))

        def give(tx, carry):
            for ty in range(4):
                for dz in range(2):
                    tz = z - rem(z, 2) + dz
                    for tc in (1, 0):
                        for t in range(tasks):
                            here = turn.at[pl.ds((t * SLABS + tx) * SLICES + (ty * 8 + tz) * 2 + tc, 1)]
                            there = back.at[pl.ds((FIELDS - 1 if t else y) * KX + scan_x2z, 1)]

                            def far():
                                pltpu.make_async_remote_copy(
                                    here, there, c_send, c_recv,
                                    device_id=at(tx, jnp.int32(ty), tz, jnp.int32(tc)), device_id_type=MESH,
                                ).start()

                            if tc == 0:
                                far()
                                continue
                            mine_too = (tx == x) & (y == ty) & (tz == z)
                            pl.when(jnp.logical_not(mine_too))(far)

                            @pl.when(mine_too)
                            def _():
                                pltpu.make_async_copy(here, there, c_recv).start()
            return carry
        lax.fori_loop(0, 4, give, 0)

    pl.when(has_two)(lambda: own(2))
    pl.when(is_owner & jnp.logical_not(has_two))(lambda: own(1))

    whole(back, ROWS, c_recv)
    back_out[...] = back[...]

    pltpu.make_async_copy(halo, halo, hs).wait()

    pass_on.wait_send()

    @pl.when(has_two)
    def _():
        whole(got, 158, f_send)
        whole(turn, 126, c_send)

    @pl.when(is_owner & jnp.logical_not(has_two))
    def _():
        whole(got, 159, f_send)
        whole(turn, 63, c_send)

    @pl.when(jnp.logical_not(is_owner))
    def _():
        whole(got, 160, f_send)

    store.wait()


def main_call(starts, source, t):
    hbm = pl.BlockSpec(memory_space=pltpu.MemorySpace.HBM)
    slab = (FIELDS, DEPTH, NY, NX)
    vm = pltpu.VMEM
    dma = pltpu.SemaphoreType.DMA
    return pl.pallas_call(
        main_kernel,
        out_shape=(jax.ShapeDtypeStruct(slab, F32), jax.ShapeDtypeStruct((ROWS, 128), F32)),
        in_specs=[hbm] * 7,
        out_specs=(pl.BlockSpec(memory_space=pl.ANY), pl.BlockSpec(memory_space=vm)),
        scratch_shapes=[
            vm(slab, F32), vm(slab, F32),
            vm((4, 10, DEPTH, FIELDS, 8, NX), F32),
            vm((4, 2, 8, FIELDS, 8, NX), F32),
            vm(slab, F32), vm(slab, F32),
            vm((32, 128), BF16), vm((2, 512, 128), BF16), vm((2, 512, 512), BF16), vm((2, 512, 512), BF16), vm((8, 512), F32),
            vm((ROWS, 128), F32), vm((ROWS, 128), F32), vm((ROWS, 128), F32),
            vm((2 * SLABS * SLICES, 128), F32), vm((2 * SLABS * SLICES, 128), F32), vm((ROWS, 128), F32),
            dma((3,)), dma((2,)), dma, dma, dma((2, 8)), pltpu.SemaphoreType.REGULAR((8,)),
            dma, dma, dma, dma, dma, dma,
        ],
        compiler_params=pltpu.CompilerParams(collective_id=0, has_side_effects=True, vmem_limit_bytes=24 << 20),
        name="fine_and_scan",
    )(
        *(
            pltpu.with_memory_space_constraint(a, pltpu.MemorySpace.HBM)
            for a in (starts, source, t["cx"], t["m1"], t["m2"], t["m3"], t["powers"])
        )
    )


def last_kernel(fine, back, m4, cinv, ends, slice_norm, total_norm, held, sem):
    rows = back[...]
    e = product(rows, m4[0], m4[1])
    copies = []
    for f in range(FIELDS):
        part = e[f * KX : (f + 1) * KX]
        high, low = split(jnp.concatenate([part[:, :256], part[:, 256:]], axis=0))
        fix = dot(jnp.concatenate([high, low, high], axis=0), cinv[...], ((0,), (0,)))
        held[f] = fine[f] + fix.reshape(DEPTH, NY, NX)
        copies.append(pltpu.make_async_copy(held.at[f], ends.at[0, f], sem))
        copies[-1].start()
    sums = jnp.sum(rows, axis=0, keepdims=True)
    cells = FIELDS * CELLS
    lane = lax.broadcasted_iota(jnp.int32, (1, 128), 1)
    one = jnp.sqrt(jnp.sum(jnp.where(lane == Q_LANE, sums, 0.0), axis=1, keepdims=True) / cells + epsilon)
    every = jnp.sqrt(jnp.sum(jnp.where(lane == T_LANE, sums, 0.0), axis=1, keepdims=True) / (cells * SLICES) + epsilon)
    slice_norm[0] = one[0, 0]
    total_norm[0] = every[0, 0]
    pltpu.make_async_copy(held, ends.at[0], sem).wait()


def last_call(fine, back, t):
    vm = pl.BlockSpec(memory_space=pltpu.VMEM)
    sm = pl.BlockSpec(memory_space=pltpu.SMEM)
    return pl.pallas_call(
        last_kernel,
        out_shape=(
            jax.ShapeDtypeStruct((1, FIELDS, DEPTH, NY, NX), F32),
            jax.ShapeDtypeStruct((1,), F32),
            jax.ShapeDtypeStruct((1,), F32),
        ),
        in_specs=[vm] * 4,
        out_specs=(pl.BlockSpec(memory_space=pltpu.MemorySpace.HBM), sm, sm),
        scratch_shapes=[pltpu.VMEM((FIELDS, DEPTH, NY, NX), F32), pltpu.SemaphoreType.DMA],
        compiler_params=pltpu.CompilerParams(vmem_limit_bytes=8 << 20),
        name="inverse_and_add",
    )(fine, back, t["m4"], t["cinv"])


def solution(mesh):
    held = Mesh(mesh.devices.reshape(4, 8, 2, mesh.shape["space"]), (*TM, X))
    t = tables()

    def shards(starts, source):
        local = {k: jnp.asarray(v) for k, v in t.items()}
        fine, back = main_call(starts, source, local)
        return last_call(fine, back, local)

    return jax.shard_map(
        shards,
        mesh=held,
        in_specs=(P(TM, None, X, None, None), P(None, X, None, None)),
        out_specs=(P(TM, None, X, None, None), P(TM), P()),
        check_vma=False,
    )
```

```python
import functools
import math

import jax
import jax.numpy as jnp
import numpy as np
from jax import lax
from jax.experimental import pallas as pl
from jax.experimental.pallas import tpu as pltpu
from jax.sharding import Mesh
from jax.sharding import PartitionSpec as P

Y, Z, C, X = "tm_0", "tm_1", "tm_2", "space"
TM = (Y, Z, C)
MESH = pl.DeviceIdType.MESH
F32, BF16 = jnp.float32, jnp.bfloat16

FIELDS, NZ, NY, NX, SLICES = 5, 16, 64, 128, 64
SLABS, DEPTH = 4, 4
KX, KY = NX // 16, NY // 8
CELLS = NZ * NY * NX
viscosity, diffusivity, compress_rate = 0.08, 0.05, 0.25
time_step, diffusion_number = 0.5, 0.08
advect = {"x": 0.2, "y": 0.15, "z": 0.1}
epsilon = 1e-06
GREETINGS = (None, 2, 6, 10, 14, 18, 22, 26)
PASS_ON = 18
QUARTERS = 4
ROWS = FIELDS * KX
Q_LANE, T_LANE = 64, 72


def halves(table):
    table = np.asarray(table, np.float32)
    high = table.astype(BF16)
    low = (table - high.astype(np.float32)).astype(BF16)
    return high, low


def tables():
    kx, xs = np.arange(KX), np.arange(NX)
    ky = (np.arange(2 * KY) + KY) % (2 * KY) - KY
    keep = (ky != -KY).astype(np.float64)
    ax = 2 * np.pi / NX * np.outer(kx, xs)
    cx = np.concatenate([np.cos(ax), np.sin(ax)])
    weight = np.where(kx == 0, 1.0, 2.0)[:, None]
    cinv = np.concatenate([weight * np.cos(ax), weight * np.sin(ax)])
    permuted = np.arange(NY).reshape(8, 8).T.reshape(-1)
    eye = np.eye(DEPTH)

    def plane(ys):
        ay = 2 * np.pi / NY * np.outer(ys, ky)
        return np.cos(ay) * keep, np.sin(ay) * keep

    co, si = plane(permuted)
    m1 = np.zeros((2, DEPTH, NY, DEPTH, 2, 2 * KY))
    for cs, (re, im) in enumerate(((co, -si), (-si, -co))):
        m1[cs, :, :, :, 0, :] = np.einsum("ab,yk->aybk", eye, re)
        m1[cs, :, :, :, 1, :] = np.einsum("ab,yk->aybk", eye, im)
    co, si = plane(np.arange(NY))
    m4 = np.zeros((DEPTH, 2, 2 * KY, 2, DEPTH, NY))
    for cs, (re, im) in enumerate(((co, -si), (-si, -co))):
        m4[:, 0, :, cs, :, :] = np.einsum("ab,yk->akby", eye, re) / CELLS
        m4[:, 1, :, cs, :, :] = np.einsum("ab,yk->akby", eye, im) / CELLS
    m1 = m1.reshape(512, DEPTH, 2, QUARTERS, 4).transpose(0, 3, 1, 2, 4)
    m4 = m4.reshape(DEPTH, 2, QUARTERS, 4, 512).transpose(2, 0, 1, 3, 4)
    zs, kz = np.arange(NZ), np.arange(NZ)
    az = 2 * np.pi / NZ * np.outer(zs, kz)
    same = np.eye(2 * KY) * keep
    m2 = np.zeros((NZ, 2, 2 * KY, 2, NZ, 2 * KY))
    m3 = np.zeros((2, NZ, 2 * KY, NZ, 2, 2 * KY))
    for i, o, fwd in ((0, 0, np.cos(az)), (0, 1, -np.sin(az)), (1, 0, np.sin(az)), (1, 1, np.cos(az))):
        m2[:, i, :, o, :, :] = np.einsum("zq,kl->zkql", fwd, same)
        m3[o, :, :, :, i, :] = np.einsum("zq,kl->qkzl", fwd, same)
    kzs = (kz + NZ // 2) % NZ - NZ // 2
    tz, ty = 2 * np.pi / NZ * kzs, 2 * np.pi / NY * ky
    tx = 2 * np.pi / NX * kx
    real = 1.0 + diffusion_number * (
        (2 * np.cos(tz) - 2)[None, :, None] + (2 * np.cos(ty) - 2)[None, None, :] + (2 * np.cos(tx) - 2)[:, None, None]
    )
    imag = -(
        advect["z"] * np.sin(tz)[None, :, None] + advect["y"] * np.sin(ty)[None, None, :] + advect["x"] * np.sin(tx)[:, None, None]
    )
    g = ((real + 1j * imag) * keep).reshape(KX, NZ * 2 * KY)
    powers = np.zeros((KX, 8, 2 * NZ * 2 * KY))
    for p in range(6):
        power = g ** (2**p)
        powers[:, p] = np.concatenate([power.real, power.imag], axis=1)
    m2 = m2.reshape(SLABS, DEPTH, 2, QUARTERS, 4, 512).transpose(0, 3, 1, 2, 4, 5)
    m3 = m3.reshape(512, SLABS, DEPTH, 2, QUARTERS, 4).transpose(0, 1, 4, 2, 3, 5)
    return dict(
        cx=np.concatenate(halves(cx)),
        m1=np.stack(halves(m1.reshape(512, 128))),
        m2=np.stack(halves(m2.reshape(512, 512))),
        m3=np.stack(halves(m3.reshape(512, 512))),
        powers=powers.astype(np.float32),
        m4=np.stack(halves(m4.reshape(128, 512))),
        cinv=np.concatenate([halves(cinv)[0], halves(cinv)[0], halves(cinv)[1]]),
    )


def split(x):
    high = x.astype(BF16)
    return high, (x - high.astype(F32)).astype(BF16)


def dot(a, b, dims=((1,), (0,))):
    return lax.dot_general(a, b, (dims, ((), ())), preferred_element_type=F32)


def product(x, high, low):
    m = x.shape[0]
    xh, xl = split(x)
    both = dot(jnp.concatenate([xh, xl], axis=0), high)
    return both[:m] + both[m:] + dot(xh, low)


def low_modes(field_rows, cx, m1):
    out = []
    for f in range(FIELDS):
        high, low = split(field_rows(f))
        a = dot(cx, high, ((1,), (1,)))
        a = a[:16] + a[16:] + dot(cx[:16], low, ((1,), (1,)))
        out.append(jnp.concatenate([a[:KX], a[KX:]], axis=1))
    return product(jnp.concatenate(out, axis=0), m1[0], m1[1])


def rem(a, n):
    return lax.rem(a, jnp.int32(n))


def picked(i, values):
    out = jnp.int32(values[-1])
    for k, v in enumerate(values[:-1]):
        out = jnp.where(i == k, jnp.int32(v), out)
    return out


def main_kernel(
    starts, source, cx_h, m1_h, m2_h, m3_h, pw_h,
    fine_out, back_out,
    st, sr, q, halo, fo, fn, cx, m1, m2, m3, pw,
    spec_s, after, spec_f, got, turn, back,
    in_sem, const_sem, out_sem, hs, hr, rounds, p_send, p_recv, f_send, f_recv, c_send, c_recv,
):
    x, y, z, c = (lax.axis_index(a) for a in (X, Y, Z, C))
    at = lambda x=x, y=y, z=z, c=c: {Y: y, Z: z, C: c, X: x}
    up, down = at(x=rem(x + 1, 4)), at(x=rem(x + 3, 4))
    load_s = [
        pltpu.make_async_copy(starts.at[0, :, pl.ds(p, n)], st.at[:, pl.ds(p, n)], in_sem.at[i])
        for i, (p, n) in ((0, (0, 1)), (0, (3, 1)), (1, (1, 2)))
    ]
    load_r = pltpu.make_async_copy(source, sr, in_sem.at[2])
    for copy in load_s[:2]:
        copy.start()
    consts = [
        pltpu.make_async_copy(a, b, const_sem.at[i])
        for i, (a, b) in ((0, (cx_h, cx)), (0, (m1_h, m1)), (1, (m2_h, m2)), (1, (m3_h, m3)))
    ]
    scan_x2z = x * 2 + rem(z, 2)
    load_p = pltpu.make_async_copy(pw_h.at[scan_x2z], pw, const_sem.at[1])

    barrier = pltpu.get_barrier_semaphore()
    around = [
        up, down, at(y=rem(y + 1, 4)), at(y=rem(y + 3, 4)), at(z=rem(z + 1, 8)), at(z=rem(z + 7, 8)), at(c=1 - c),
    ]
    for device in around:
        pl.semaphore_signal(barrier, inc=1, device_id=device, device_id_type=MESH)

    def greet(k):
        for turn_by in (1, -1):
            device = (
                at(x=rem(x + turn_by + 4, 4)), at(c=1 - c),
                at(y=rem(y + turn_by + 4, 4)), at(y=rem(y + turn_by + 4, 4)),
                *[at(z=rem(z + turn_by + 8, 8))] * 4,
            )[k]
            pl.semaphore_signal(rounds.at[k], inc=1, device_id=device, device_id_type=MESH)

    load_s[0].wait()
    load_s[1].wait()
    load_s[2].start()

    def lay(planes):
        def body(r, carry):
            for plane in planes:
                for f in range(FIELDS):
                    q[0, r + 1, plane, f] = st[f, plane, pl.ds(r, 8, stride=8), :]
            return carry
        lax.fori_loop(0, 8, body, 0)

    def edges(j, last):
        for plane in range(DEPTH):
            for f in range(FIELDS):
                if last:
                    q[j, 0, plane, f] = pltpu.roll(q[j, 8, plane, f], 1, 0)
                else:
                    q[j, 9, plane, f] = pltpu.roll(q[j, 1, plane, f], 7, 0)

    def sends(j, r):
        return (
            pltpu.make_async_remote_copy(
                q.at[j, r + 1, 0], halo.at[j, 1, r], hs, hr.at[j % 2, r], device_id=down, device_id_type=MESH
            ),
            pltpu.make_async_remote_copy(
                q.at[j, r + 1, DEPTH - 1], halo.at[j, 0, r], hs, hr.at[j % 2, r], device_id=up, device_id_type=MESH
            ),
        )

    lay((0, 3))
    pl.semaphore_wait(barrier, len(around))
    greet(0)

    def first(r, carry):
        for copy in sends(0, r):
            copy.start()
        return carry
    lax.fori_loop(0, 8, first, 0)
    for copy in (*consts[:2], load_r, *consts[2:], load_p):
        copy.start()
    load_s[2].wait()
    lay((1, 2))
    edges(0, False)
    edges(0, True)

    consts[0].wait()
    consts[1].wait()
    spec_s[...] = low_modes(
        lambda f: jnp.concatenate([q[0, 1:9, p, f].reshape(NY, NX) for p in range(DEPTH)], axis=0), cx[...], m1
    )
    load_r.wait()

    is_owner = c == 1
    has_two = is_owner & (y == 0)
    mine = (y * 8 + z) * 2 + c

    before = rem(mine + SLICES - 1, SLICES)
    pass_on = pltpu.make_async_remote_copy(
        spec_s, after, p_send, p_recv,
        device_id=at(y=lax.div(before, jnp.int32(16)), z=rem(lax.div(before, jnp.int32(2)), 8), c=rem(before, 2)),
        device_id_type=MESH,
    )

    def spread(tz):
        slot = x * SLICES + rem(mine + 1, SLICES)
        for dx in (2, 1, 3, 0):
            tx = rem(x + dx, 4)
            kx = tx * 2 + rem(tz, 2)
            for dy in (2, 1, 3, 0, None):
                ty = jnp.int32(0) if dy is None else rem(y + dy, 4)
                row = (32 if dy is None else ty * KX) + kx
                here = spec_f.at[pl.ds(row, 1)]
                there = got.at[pl.ds(slot + (SLABS * SLICES if dy is None else 0), 1)]

                def far():
                    pltpu.make_async_remote_copy(
                        here, there, f_send, f_recv, device_id=at(tx, ty, tz, jnp.int32(1)), device_id_type=MESH
                    ).start()

                if dx or dy:
                    far()
                    continue
                own = (tz == z) & (ty == y) & is_owner
                pl.when(jnp.logical_not(own))(far)

                @pl.when(own)
                def _():
                    pltpu.make_async_copy(here, there, f_recv).start()

    def stage(j):
        def body(i, carry):
            r = rem(i + j, 8)
            pltpu.make_async_copy(halo.at[j, :, r], halo.at[j, :, r], hr.at[j % 2, r]).wait()
            for k, turn_at in enumerate(GREETINGS):
                if turn_at is None or turn_at // 8 != j:
                    continue

                @pl.when(i == turn_at % 8)
                def _():
                    pl.semaphore_wait(rounds.at[k - 1], 2)
                    greet(k)
                    if turn_at == PASS_ON:
                        pass_on.start()

            for plane in (0, 3, 1, 2):
                cur = [q[j, r + 1, plane, f] for f in range(FIELDS)]
                yp = [q[j, r + 2, plane, f] for f in range(FIELDS)]
                ym = [q[j, r, plane, f] for f in range(FIELDS)]
                zp = [(halo[j, 1, r, f] if plane == 3 else q[j, r + 1, plane + 1, f]) for f in range(FIELDS)]
                zm = [(halo[j, 0, r, f] if plane == 0 else q[j, r + 1, plane - 1, f]) for f in range(FIELDS)]

                def flux(v, axis, sign):
                    half = 0.5 * advect["xyz"[axis]] + 0.5 * v[axis]
                    a = viscosity - half if sign > 0 else viscosity + half
                    b = diffusivity - half if sign > 0 else diffusivity + half
                    out = [a * v[0], a * v[1], a * v[2], b * v[4]]
                    push = 0.5 * v[3]
                    out[axis] = out[axis] - push if sign > 0 else out[axis] + push
                    return out

                xplus = [pltpu.roll(v, NX - 1, 1) for v in flux(cur, 0, 1)]
                xminus = [pltpu.roll(v, 1, 1) for v in flux(cur, 0, -1)]
                parts = (xplus, xminus, flux(yp, 1, 1), flux(ym, 1, -1), flux(zp, 2, 1), flux(zm, 2, -1))
                diverge = (
                    (pltpu.roll(cur[0], NX - 1, 1) - pltpu.roll(cur[0], 1, 1)) + (yp[1] - ym[1]) + (zp[2] - zm[2])
                )
                src = [sr[f, plane, pl.ds(r, 8, stride=8), :] for f in range(FIELDS)]
                rates = [None] * FIELDS
                for n, f in enumerate((0, 1, 2, 4)):
                    coefficient = -6.0 * (viscosity if f < 3 else diffusivity)
                    total = coefficient * cur[f] + src[f]
                    pairs = [p[n] for p in parts]
                    rates[f] = total + ((pairs[0] + pairs[1]) + (pairs[2] + pairs[3]) + (pairs[4] + pairs[5]))
                rates[3] = src[3] - (0.5 * compress_rate) * diverge
                for f in range(FIELDS):
                    begin = q[0, r + 1, plane, f]
                    if j < 3:
                        step = time_step * (0.5 if j < 2 else 1.0)
                        q[j + 1, r + 1, plane, f] = begin + step * rates[f]
                    else:
                        two = q[2, r + 1, plane, f]
                        states = (q[1, r + 1, plane, f] + two) + (two + cur[f]) - begin
                        fo[f, plane, pl.ds(pl.multiple_of(r * 8, 8), 8), :] = (1.0 / 3.0) * states + (
                            time_step / 6.0
                        ) * rates[f]
            if j < 3:
                for copy in sends(j + 1, r):
                    copy.start()
                pl.when(r == 0)(lambda: edges(j + 1, False))
                pl.when(r == 7)(lambda: edges(j + 1, True))
            return carry
        lax.fori_loop(0, 8, body, 0)

    for j in range(4):
        stage(j)
    pl.semaphore_wait(rounds.at[7], 2)

    modes = low_modes(lambda f: fo[f].reshape(DEPTH * NY, NX), cx[...], m1)
    pass_on.wait_recv()
    spec_f[...] = modes - after[...]

    def fine_rows(i, carry):
        spread(picked(i, (0, 1, 7, 2, 6, 3, 5, 4)))
        return carry
    lax.fori_loop(0, 8, fine_rows, 0)

    def plain(a, carry):
        for f in range(FIELDS):
            for p in range(DEPTH):
                fn[f, p, pl.ds(pl.multiple_of(a * 8, 8), 8), :] = fo[f, p, pl.ds(a, 8, stride=8), :]
        return carry
    lax.fori_loop(0, 8, plain, 0)
    store = pltpu.make_async_copy(fn, fine_out, out_sem)
    store.start()
    consts[2].wait()
    consts[3].wait()
    load_p.wait()

    def whole(ref, n, sem):
        pltpu.make_async_copy(ref.at[pl.ds(0, n)], ref.at[pl.ds(0, n)], sem).wait()

    def own(tasks):
        whole(got, tasks * SLABS * SLICES, f_recv)
        later = lax.broadcasted_iota(jnp.int32, (SLICES, 128), 0) > 0
        blocks = []
        for t in range(tasks):
            at_row = lambda s: (t * SLABS + s) * SLICES
            jumps = [jnp.where(later, got[at_row(s) : at_row(s) + SLICES], 0.0) for s in range(SLABS)]
            blocks.append(jnp.concatenate(jumps, axis=1))
        modes = product(jnp.concatenate(blocks, axis=0), m2[0], m2[1])
        half = NZ * 2 * KY

        def times(p, re, im):
            gr, gi = pw[p : p + 1, :half], pw[p : p + 1, half:]
            return gr * re - gi * im, gr * im + gi * re

        weight = jnp.where(scan_x2z == 0, 1.0, 2.0) / CELLS
        fixes, sums = [], []
        for t in range(tasks):
            one = modes[t * SLICES : (t + 1) * SLICES]
            re, im = times(0, one[:, :half], one[:, half:])
            for p in range(6):
                zero = jnp.zeros((2**p, half), F32)
                shifted = (jnp.concatenate([zero, v[: -(2**p)]], axis=0) for v in (re, im))
                pr, pi = times(p, *shifted)
                re, im = re + pr, im + pi
            sums.append(jnp.sum(re * re + im * im, axis=1, keepdims=True) * weight)
            fixes.append(jnp.concatenate([re, im], axis=1))
        out = product(jnp.concatenate(fixes, axis=0), m3[0], m3[1])
        lane = lax.broadcasted_iota(jnp.int32, (SLICES, 128), 1)
        for t in range(tasks):
            total = jnp.sum(sums[t], axis=0, keepdims=True)
            for s in range(SLABS):
                piece = out[t * SLICES : (t + 1) * SLICES, s * 128 : (s + 1) * 128]
                row = (t * SLABS + s) * SLICES
                turn[row : row + SLICES] = jnp.where(lane == T_LANE, total, jnp.where(lane == Q_LANE, sums[t], piece))

        def give(tx, carry):
            for ty in range(4):
                for dz in range(2):
                    tz = z - rem(z, 2) + dz
                    for tc in (1, 0):
                        for t in range(tasks):
                            here = turn.at[pl.ds((t * SLABS + tx) * SLICES + (ty * 8 + tz) * 2 + tc, 1)]
                            there = back.at[pl.ds((FIELDS - 1 if t else y) * KX + scan_x2z, 1)]

                            def far():
                                pltpu.make_async_remote_copy(
                                    here, there, c_send, c_recv,
                                    device_id=at(tx, jnp.int32(ty), tz, jnp.int32(tc)), device_id_type=MESH,
                                ).start()

                            if tc == 0:
                                far()
                                continue
                            mine_too = (tx == x) & (y == ty) & (tz == z)
                            pl.when(jnp.logical_not(mine_too))(far)

                            @pl.when(mine_too)
                            def _():
                                pltpu.make_async_copy(here, there, c_recv).start()
            return carry
        lax.fori_loop(0, 4, give, 0)

    pl.when(has_two)(lambda: own(2))
    pl.when(is_owner & jnp.logical_not(has_two))(lambda: own(1))

    whole(back, ROWS, c_recv)
    back_out[...] = back[...]

    pltpu.make_async_copy(halo, halo, hs).wait()

    pass_on.wait_send()

    @pl.when(has_two)
    def _():
        whole(got, 158, f_send)
        whole(turn, 126, c_send)

    @pl.when(is_owner & jnp.logical_not(has_two))
    def _():
        whole(got, 159, f_send)
        whole(turn, 63, c_send)

    @pl.when(jnp.logical_not(is_owner))
    def _():
        whole(got, 160, f_send)

    store.wait()


def main_call(starts, source, t):
    hbm = pl.BlockSpec(memory_space=pltpu.MemorySpace.HBM)
    slab = (FIELDS, DEPTH, NY, NX)
    vm = pltpu.VMEM
    dma = pltpu.SemaphoreType.DMA
    return pl.pallas_call(
        main_kernel,
        out_shape=(jax.ShapeDtypeStruct(slab, F32), jax.ShapeDtypeStruct((ROWS, 128), F32)),
        in_specs=[hbm] * 7,
        out_specs=(pl.BlockSpec(memory_space=pl.ANY), pl.BlockSpec(memory_space=vm)),
        scratch_shapes=[
            vm(slab, F32), vm(slab, F32),
            vm((4, 10, DEPTH, FIELDS, 8, NX), F32),
            vm((4, 2, 8, FIELDS, 8, NX), F32),
            vm(slab, F32), vm(slab, F32),
            vm((32, 128), BF16), vm((2, 512, 128), BF16), vm((2, 512, 512), BF16), vm((2, 512, 512), BF16), vm((8, 512), F32),
            vm((ROWS, 128), F32), vm((ROWS, 128), F32), vm((ROWS, 128), F32),
            vm((2 * SLABS * SLICES, 128), F32), vm((2 * SLABS * SLICES, 128), F32), vm((ROWS, 128), F32),
            dma((3,)), dma((2,)), dma, dma, dma((2, 8)), pltpu.SemaphoreType.REGULAR((8,)),
            dma, dma, dma, dma, dma, dma,
        ],
        compiler_params=pltpu.CompilerParams(collective_id=0, has_side_effects=True, vmem_limit_bytes=24 << 20),
        name="fine_and_scan",
    )(
        *(
            pltpu.with_memory_space_constraint(a, pltpu.MemorySpace.HBM)
            for a in (starts, source, t["cx"], t["m1"], t["m2"], t["m3"], t["powers"])
        )
    )


def last_kernel(fine, back, m4, cinv, ends, slice_norm, total_norm, held, norms, sem, norm_sem):
    rows = back[...]
    sums = jnp.sum(rows, axis=0, keepdims=True)
    cells = FIELDS * CELLS
    lane = lax.broadcasted_iota(jnp.int32, (1, 128), 1)
    one = jnp.sqrt(jnp.sum(jnp.where(lane == Q_LANE, sums, 0.0), axis=1, keepdims=True) / cells + epsilon)
    every = jnp.sqrt(jnp.sum(jnp.where(lane == T_LANE, sums, 0.0), axis=1, keepdims=True) / (cells * SLICES) + epsilon)
    norms[0, 0] = one[0, 0]
    norms[1, 0] = every[0, 0]
    norm_copies = [
        pltpu.make_async_copy(norms.at[i], out, norm_sem.at[i]) for i, out in enumerate((slice_norm, total_norm))
    ]
    for copy in norm_copies:
        copy.start()
    e = product(rows, m4[0], m4[1])
    copies = []
    for f in range(FIELDS):
        part = e[f * KX : (f + 1) * KX]
        high, low = split(jnp.concatenate([part[:, :256], part[:, 256:]], axis=0))
        fix = dot(jnp.concatenate([high, low, high], axis=0), cinv[...], ((0,), (0,)))
        held[f] = fine[f] + fix.reshape(DEPTH, NY, NX)
        copies.append(pltpu.make_async_copy(held.at[f], ends.at[0, f], sem))
        copies[-1].start()
    pltpu.make_async_copy(held, ends.at[0], sem).wait()
    for copy in norm_copies:
        copy.wait()


def last_call(fine, back, t):
    vm = pl.BlockSpec(memory_space=pltpu.VMEM)
    hbm = pl.BlockSpec(memory_space=pltpu.MemorySpace.HBM)
    return pl.pallas_call(
        last_kernel,
        out_shape=(
            jax.ShapeDtypeStruct((1, FIELDS, DEPTH, NY, NX), F32),
            jax.ShapeDtypeStruct((1,), F32),
            jax.ShapeDtypeStruct((1,), F32),
        ),
        in_specs=[vm] * 4,
        out_specs=(hbm, hbm, hbm),
        scratch_shapes=[
            pltpu.VMEM((FIELDS, DEPTH, NY, NX), F32), pltpu.SMEM((2, 1), F32),
            pltpu.SemaphoreType.DMA, pltpu.SemaphoreType.DMA((2,)),
        ],
        compiler_params=pltpu.CompilerParams(vmem_limit_bytes=8 << 20),
        name="inverse_and_add",
    )(fine, back, t["m4"], t["cinv"])


def solution(mesh):
    held = Mesh(mesh.devices.reshape(4, 8, 2, mesh.shape["space"]), (*TM, X))
    t = tables()

    def shards(starts, source):
        local = {k: jnp.asarray(v) for k, v in t.items()}
        fine, back = main_call(starts, source, local)
        return last_call(fine, back, local)

    return jax.shard_map(
        shards,
        mesh=held,
        in_specs=(P(TM, None, X, None, None), P(None, X, None, None)),
        out_specs=(P(TM, None, X, None, None), P(TM), P()),
        check_vma=False,
    )
```

```python
import functools
import math

import jax
import jax.numpy as jnp
import numpy as np
from jax import lax
from jax.experimental import pallas as pl
from jax.experimental.pallas import tpu as pltpu
from jax.sharding import Mesh
from jax.sharding import PartitionSpec as P

Y, Z, C, X = "tm_0", "tm_1", "tm_2", "space"
TM = (Y, Z, C)
MESH = pl.DeviceIdType.MESH
F32, BF16 = jnp.float32, jnp.bfloat16

FIELDS, NZ, NY, NX, SLICES = 5, 16, 64, 128, 64
SLABS, DEPTH = 4, 4
KX, KY = NX // 16, NY // 8
CELLS = NZ * NY * NX
viscosity, diffusivity, compress_rate = 0.08, 0.05, 0.25
time_step, diffusion_number = 0.5, 0.08
advect = {"x": 0.2, "y": 0.15, "z": 0.1}
epsilon = 1e-06
GREETINGS = (None, 1, 5, 10, 15, 19, 23, 27)
PASS_ON = 19
QUARTERS = 4
ROWS = FIELDS * KX
Q_LANE, T_LANE = 64, 72


def halves(table):
    table = np.asarray(table, np.float32)
    high = table.astype(BF16)
    low = (table - high.astype(np.float32)).astype(BF16)
    return high, low


def tables():
    kx, xs = np.arange(KX), np.arange(NX)
    ky = (np.arange(2 * KY) + KY) % (2 * KY) - KY
    keep = (ky != -KY).astype(np.float64)
    ax = 2 * np.pi / NX * np.outer(kx, xs)
    cx = np.concatenate([np.cos(ax), np.sin(ax)])
    weight = np.where(kx == 0, 1.0, 2.0)[:, None]
    cinv = np.concatenate([weight * np.cos(ax), weight * np.sin(ax)])
    permuted = np.arange(NY).reshape(8, 8).T.reshape(-1)
    eye = np.eye(DEPTH)

    def plane(ys):
        ay = 2 * np.pi / NY * np.outer(ys, ky)
        return np.cos(ay) * keep, np.sin(ay) * keep

    co, si = plane(permuted)
    m1 = np.zeros((2, DEPTH, NY, DEPTH, 2, 2 * KY))
    for cs, (re, im) in enumerate(((co, -si), (-si, -co))):
        m1[cs, :, :, :, 0, :] = np.einsum("ab,yk->aybk", eye, re)
        m1[cs, :, :, :, 1, :] = np.einsum("ab,yk->aybk", eye, im)
    co, si = plane(np.arange(NY))
    m4 = np.zeros((DEPTH, 2, 2 * KY, 2, DEPTH, NY))
    for cs, (re, im) in enumerate(((co, -si), (-si, -co))):
        m4[:, 0, :, cs, :, :] = np.einsum("ab,yk->akby", eye, re) / CELLS
        m4[:, 1, :, cs, :, :] = np.einsum("ab,yk->akby", eye, im) / CELLS
    m1 = m1.reshape(512, DEPTH, 2, QUARTERS, 4).transpose(0, 3, 1, 2, 4)
    m4 = m4.reshape(DEPTH, 2, QUARTERS, 4, 512).transpose(2, 0, 1, 3, 4)
    zs, kz = np.arange(NZ), np.arange(NZ)
    az = 2 * np.pi / NZ * np.outer(zs, kz)
    same = np.eye(2 * KY) * keep
    m2 = np.zeros((NZ, 2, 2 * KY, 2, NZ, 2 * KY))
    m3 = np.zeros((2, NZ, 2 * KY, NZ, 2, 2 * KY))
    for i, o, fwd in ((0, 0, np.cos(az)), (0, 1, -np.sin(az)), (1, 0, np.sin(az)), (1, 1, np.cos(az))):
        m2[:, i, :, o, :, :] = np.einsum("zq,kl->zkql", fwd, same)
        m3[o, :, :, :, i, :] = np.einsum("zq,kl->qkzl", fwd, same)
    kzs = (kz + NZ // 2) % NZ - NZ // 2
    tz, ty = 2 * np.pi / NZ * kzs, 2 * np.pi / NY * ky
    tx = 2 * np.pi / NX * kx
    real = 1.0 + diffusion_number * (
        (2 * np.cos(tz) - 2)[None, :, None] + (2 * np.cos(ty) - 2)[None, None, :] + (2 * np.cos(tx) - 2)[:, None, None]
    )
    imag = -(
        advect["z"] * np.sin(tz)[None, :, None] + advect["y"] * np.sin(ty)[None, None, :] + advect["x"] * np.sin(tx)[:, None, None]
    )
    g = ((real + 1j * imag) * keep)[:, [*range(0, NZ, 2), *range(1, NZ, 2)]].reshape(KX, NZ * 2 * KY)
    powers = np.zeros((KX, 8, 2 * NZ * 2 * KY))
    for p in range(6):
        power = g ** (2**p)
        powers[:, p] = np.concatenate([power.real, power.imag], axis=1)
    m2 = m2.reshape(SLABS, DEPTH, 2, QUARTERS, 4, 512).transpose(0, 3, 1, 2, 4, 5).reshape(SLABS, 128, 2, NZ, 2 * KY)
    m3 = m3.reshape(512, SLABS, DEPTH, 2, QUARTERS, 4).transpose(0, 1, 4, 2, 3, 5).reshape(2, NZ, 2 * KY, SLABS, 128)
    m2 = np.stack([m2[:2, :, :, odd::2].reshape(256, 256) for odd in range(2)])
    m3 = np.stack([m3[:, odd::2, :, :2].reshape(256, 256) for odd in range(2)])
    return dict(
        cx=np.concatenate(halves(cx)),
        m1=np.stack(halves(m1.reshape(512, 128))),
        m2=np.stack(halves(m2)),
        m3=np.stack(halves(m3)),
        powers=powers.astype(np.float32),
        m4=np.stack(halves(m4.reshape(128, 512))),
        cinv=np.concatenate([halves(cinv)[0], halves(cinv)[0], halves(cinv)[1]]),
    )


def split(x):
    high = x.astype(BF16)
    return high, (x - high.astype(F32)).astype(BF16)


def dot(a, b, dims=((1,), (0,))):
    return lax.dot_general(a, b, (dims, ((), ())), preferred_element_type=F32)


def product(x, high, low):
    m = x.shape[0]
    xh, xl = split(x)
    both = dot(jnp.concatenate([xh, xl], axis=0), high)
    return both[:m] + both[m:] + dot(xh, low)


def low_modes(field_rows, cx, m1):
    out = []
    for f in range(FIELDS):
        high, low = split(field_rows(f))
        a = dot(cx, high, ((1,), (1,)))
        a = a[:16] + a[16:] + dot(cx[:16], low, ((1,), (1,)))
        out.append(jnp.concatenate([a[:KX], a[KX:]], axis=1))
    return product(jnp.concatenate(out, axis=0), m1[0], m1[1])


def rem(a, n):
    return lax.rem(a, jnp.int32(n))


def picked(i, values):
    out = jnp.int32(values[-1])
    for k, v in enumerate(values[:-1]):
        out = jnp.where(i == k, jnp.int32(v), out)
    return out


def main_kernel(
    starts, source, cx_h, m1_h, m2_h, m3_h, pw_h,
    fine_out, back_out,
    st, sr, q, halo, fo, fn, cx, m1, m2, m3, pw,
    spec_s, after, spec_f, got, turn, back,
    in_sem, const_sem, out_sem, hs, hr, rounds, p_send, p_recv, f_send, f_recv, c_send, c_recv,
):
    x, y, z, c = (lax.axis_index(a) for a in (X, Y, Z, C))
    at = lambda x=x, y=y, z=z, c=c: {Y: y, Z: z, C: c, X: x}
    up, down = at(x=rem(x + 1, 4)), at(x=rem(x + 3, 4))
    load_s = [
        pltpu.make_async_copy(starts.at[0, :, pl.ds(p, n)], st.at[:, pl.ds(p, n)], in_sem.at[i])
        for i, (p, n) in ((0, (0, 1)), (0, (3, 1)), (1, (1, 2)))
    ]
    load_r = pltpu.make_async_copy(source, sr, in_sem.at[2])
    for copy in load_s[:2]:
        copy.start()
    consts = [
        pltpu.make_async_copy(a, b, const_sem.at[i])
        for i, (a, b) in ((0, (cx_h, cx)), (0, (m1_h, m1)), (1, (m2_h, m2)), (1, (m3_h, m3)))
    ]
    scan_x2z = x * 2 + rem(z, 2)
    load_p = pltpu.make_async_copy(pw_h.at[scan_x2z], pw, const_sem.at[1])

    barrier = pltpu.get_barrier_semaphore()
    around = [
        up, down, at(y=rem(y + 1, 4)), at(y=rem(y + 3, 4)), at(z=rem(z + 1, 8)), at(z=rem(z + 7, 8)), at(c=1 - c),
    ]
    for device in around:
        pl.semaphore_signal(barrier, inc=1, device_id=device, device_id_type=MESH)

    def greet(k):
        for turn_by in (1, -1):
            device = (
                at(x=rem(x + turn_by + 4, 4)), at(c=1 - c),
                at(y=rem(y + turn_by + 4, 4)), at(y=rem(y + turn_by + 4, 4)),
                *[at(z=rem(z + turn_by + 8, 8))] * 4,
            )[k]
            pl.semaphore_signal(rounds.at[k], inc=1, device_id=device, device_id_type=MESH)

    load_s[0].wait()
    load_s[1].wait()
    load_s[2].start()

    def lay(planes):
        def body(r, carry):
            for plane in planes:
                for f in range(FIELDS):
                    q[0, r + 1, plane, f] = st[f, plane, pl.ds(r, 8, stride=8), :]
            return carry
        lax.fori_loop(0, 8, body, 0)

    def edges(j, last):
        for plane in range(DEPTH):
            for f in range(FIELDS):
                if last:
                    q[j, 0, plane, f] = pltpu.roll(q[j, 8, plane, f], 1, 0)
                else:
                    q[j, 9, plane, f] = pltpu.roll(q[j, 1, plane, f], 7, 0)

    def sends(j, r):
        return (
            pltpu.make_async_remote_copy(
                q.at[j, r + 1, 0], halo.at[j, 1, r], hs, hr.at[j % 2, r], device_id=down, device_id_type=MESH
            ),
            pltpu.make_async_remote_copy(
                q.at[j, r + 1, DEPTH - 1], halo.at[j, 0, r], hs, hr.at[j % 2, r], device_id=up, device_id_type=MESH
            ),
        )

    lay((0, 3))
    pl.semaphore_wait(barrier, len(around))
    greet(0)

    def first(r, carry):
        for copy in sends(0, r):
            copy.start()
        return carry
    lax.fori_loop(0, 8, first, 0)
    for copy in (*consts[:2], load_r, *consts[2:], load_p):
        copy.start()
    load_s[2].wait()
    lay((1, 2))
    edges(0, False)
    edges(0, True)

    consts[0].wait()
    consts[1].wait()
    spec_s[...] = low_modes(
        lambda f: jnp.concatenate([q[0, 1:9, p, f].reshape(NY, NX) for p in range(DEPTH)], axis=0), cx[...], m1
    )
    load_r.wait()

    is_owner = c == 1
    has_two = is_owner & (y == 0)
    mine = (y * 8 + z) * 2 + c

    before = rem(mine + SLICES - 1, SLICES)
    pass_on = pltpu.make_async_remote_copy(
        spec_s, after, p_send, p_recv,
        device_id=at(y=lax.div(before, jnp.int32(16)), z=rem(lax.div(before, jnp.int32(2)), 8), c=rem(before, 2)),
        device_id_type=MESH,
    )

    def spread(tz):
        slot = x * SLICES + rem(mine + 1, SLICES)
        for dx in (2, 1, 3, 0):
            tx = rem(x + dx, 4)
            kx = tx * 2 + rem(tz, 2)
            for dy in (2, 1, 3, 0, None):
                ty = jnp.int32(0) if dy is None else rem(y + dy, 4)
                row = (32 if dy is None else ty * KX) + kx
                here = spec_f.at[pl.ds(row, 1)]
                there = got.at[pl.ds(slot + (SLABS * SLICES if dy is None else 0), 1)]

                def far():
                    pltpu.make_async_remote_copy(
                        here, there, f_send, f_recv, device_id=at(tx, ty, tz, jnp.int32(1)), device_id_type=MESH
                    ).start()

                if dx or dy:
                    far()
                    continue
                own = (tz == z) & (ty == y) & is_owner
                pl.when(jnp.logical_not(own))(far)

                @pl.when(own)
                def _():
                    pltpu.make_async_copy(here, there, f_recv).start()

    def stage(j):
        def body(i, carry):
            r = rem(i + j, 8)
            pltpu.make_async_copy(halo.at[j, :, r], halo.at[j, :, r], hr.at[j % 2, r]).wait()
            for k, turn_at in enumerate(GREETINGS):
                if turn_at is None or turn_at // 8 != j:
                    continue

                @pl.when(i == turn_at % 8)
                def _():
                    pl.semaphore_wait(rounds.at[k - 1], 2)
                    greet(k)
                    if turn_at == PASS_ON:
                        pass_on.start()

            for plane in (0, 3, 1, 2):
                cur = [q[j, r + 1, plane, f] for f in range(FIELDS)]
                yp = [q[j, r + 2, plane, f] for f in range(FIELDS)]
                ym = [q[j, r, plane, f] for f in range(FIELDS)]
                zp = [(halo[j, 1, r, f] if plane == 3 else q[j, r + 1, plane + 1, f]) for f in range(FIELDS)]
                zm = [(halo[j, 0, r, f] if plane == 0 else q[j, r + 1, plane - 1, f]) for f in range(FIELDS)]

                def flux(v, axis, sign):
                    half = 0.5 * advect["xyz"[axis]] + 0.5 * v[axis]
                    a = viscosity - half if sign > 0 else viscosity + half
                    b = diffusivity - half if sign > 0 else diffusivity + half
                    out = [a * v[0], a * v[1], a * v[2], b * v[4]]
                    push = 0.5 * v[3]
                    out[axis] = out[axis] - push if sign > 0 else out[axis] + push
                    return out

                xplus = [pltpu.roll(v, NX - 1, 1) for v in flux(cur, 0, 1)]
                xminus = [pltpu.roll(v, 1, 1) for v in flux(cur, 0, -1)]
                parts = (xplus, xminus, flux(yp, 1, 1), flux(ym, 1, -1), flux(zp, 2, 1), flux(zm, 2, -1))
                diverge = (
                    (pltpu.roll(cur[0], NX - 1, 1) - pltpu.roll(cur[0], 1, 1)) + (yp[1] - ym[1]) + (zp[2] - zm[2])
                )
                src = [sr[f, plane, pl.ds(r, 8, stride=8), :] for f in range(FIELDS)]
                rates = [None] * FIELDS
                for n, f in enumerate((0, 1, 2, 4)):
                    coefficient = -6.0 * (viscosity if f < 3 else diffusivity)
                    total = coefficient * cur[f] + src[f]
                    pairs = [p[n] for p in parts]
                    rates[f] = total + ((pairs[0] + pairs[1]) + (pairs[2] + pairs[3]) + (pairs[4] + pairs[5]))
                rates[3] = src[3] - (0.5 * compress_rate) * diverge
                for f in range(FIELDS):
                    begin = q[0, r + 1, plane, f]
                    if j < 3:
                        step = time_step * (0.5 if j < 2 else 1.0)
                        q[j + 1, r + 1, plane, f] = begin + step * rates[f]
                    else:
                        two = q[2, r + 1, plane, f]
                        states = (q[1, r + 1, plane, f] + two) + (two + cur[f]) - begin
                        fo[f, plane, pl.ds(pl.multiple_of(r * 8, 8), 8), :] = (1.0 / 3.0) * states + (
                            time_step / 6.0
                        ) * rates[f]
            if j < 3:
                for copy in sends(j + 1, r):
                    copy.start()
                pl.when(r == 0)(lambda: edges(j + 1, False))
                pl.when(r == 7)(lambda: edges(j + 1, True))
            return carry
        lax.fori_loop(0, 8, body, 0)

    for j in range(4):
        stage(j)
    pl.semaphore_wait(rounds.at[7], 2)

    modes = low_modes(lambda f: fo[f].reshape(DEPTH * NY, NX), cx[...], m1)
    pass_on.wait_recv()
    spec_f[...] = modes - after[...]

    def fine_rows(i, carry):
        spread(picked(i, (0, 1, 7, 2, 6, 3, 5, 4)))
        return carry
    lax.fori_loop(0, 8, fine_rows, 0)

    def plain(a, carry):
        for f in range(FIELDS):
            for p in range(DEPTH):
                fn[f, p, pl.ds(pl.multiple_of(a * 8, 8), 8), :] = fo[f, p, pl.ds(a, 8, stride=8), :]
        return carry
    lax.fori_loop(0, 8, plain, 0)
    store = pltpu.make_async_copy(fn, fine_out, out_sem)
    store.start()
    consts[2].wait()
    consts[3].wait()
    load_p.wait()

    def whole(ref, n, sem):
        pltpu.make_async_copy(ref.at[pl.ds(0, n)], ref.at[pl.ds(0, n)], sem).wait()

    def own(tasks):
        whole(got, tasks * SLABS * SLICES, f_recv)
        later = lax.broadcasted_iota(jnp.int32, (SLICES, 128), 0) > 0
        blocks = ([], [])
        for t in range(tasks):
            at_row = lambda s: (t * SLABS + s) * SLICES
            jumps = [jnp.where(later, got[at_row(s) : at_row(s) + SLICES], 0.0) for s in range(SLABS)]
            blocks[0].append(jnp.concatenate([jumps[0] + jumps[2], jumps[1] + jumps[3]], axis=1))
            blocks[1].append(jnp.concatenate([jumps[0] - jumps[2], jumps[1] - jumps[3]], axis=1))
        even, odd = (product(jnp.concatenate(blocks[i], axis=0), m2[0, i], m2[1, i]) for i in range(2))
        half = NZ * 2 * KY

        def times(p, re, im):
            gr, gi = pw[p : p + 1, :half], pw[p : p + 1, half:]
            return gr * re - gi * im, gr * im + gi * re

        weight = jnp.where(scan_x2z == 0, 1.0, 2.0) / CELLS
        fixes, sums = [], []
        for t in range(tasks):
            parts = [v[t * SLICES : (t + 1) * SLICES] for v in (even, odd)]
            re, im = times(0, *(jnp.concatenate([v[:, i : i + 128] for v in parts], axis=1) for i in (0, 128)))
            for p in range(6):
                zero = jnp.zeros((2**p, half), F32)
                shifted = (jnp.concatenate([zero, v[: -(2**p)]], axis=0) for v in (re, im))
                pr, pi = times(p, *shifted)
                re, im = re + pr, im + pi
            sums.append(jnp.sum(re * re + im * im, axis=1, keepdims=True) * weight)
            fixes.append([jnp.concatenate([re[:, i : i + 128], im[:, i : i + 128]], axis=1) for i in (0, 128)])
        even, odd = (product(jnp.concatenate([v[i] for v in fixes], axis=0), m3[0, i], m3[1, i]) for i in range(2))
        out = (even + odd, even - odd)
        lane = lax.broadcasted_iota(jnp.int32, (SLICES, 128), 1)
        for t in range(tasks):
            total = jnp.sum(sums[t], axis=0, keepdims=True)
            for s in range(SLABS):
                piece = out[s // 2][t * SLICES : (t + 1) * SLICES, s % 2 * 128 : s % 2 * 128 + 128]
                row = (t * SLABS + s) * SLICES
                turn[row : row + SLICES] = jnp.where(lane == T_LANE, total, jnp.where(lane == Q_LANE, sums[t], piece))

        def give(tx, carry):
            for ty in range(4):
                for dz in range(2):
                    tz = z - rem(z, 2) + dz
                    for tc in (1, 0):
                        for t in range(tasks):
                            here = turn.at[pl.ds((t * SLABS + tx) * SLICES + (ty * 8 + tz) * 2 + tc, 1)]
                            there = back.at[pl.ds((FIELDS - 1 if t else y) * KX + scan_x2z, 1)]

                            def far():
                                pltpu.make_async_remote_copy(
                                    here, there, c_send, c_recv,
                                    device_id=at(tx, jnp.int32(ty), tz, jnp.int32(tc)), device_id_type=MESH,
                                ).start()

                            if tc == 0:
                                far()
                                continue
                            mine_too = (tx == x) & (y == ty) & (tz == z)
                            pl.when(jnp.logical_not(mine_too))(far)

                            @pl.when(mine_too)
                            def _():
                                pltpu.make_async_copy(here, there, c_recv).start()
            return carry
        lax.fori_loop(0, 4, give, 0)

    pl.when(has_two)(lambda: own(2))
    pl.when(is_owner & jnp.logical_not(has_two))(lambda: own(1))

    whole(back, ROWS, c_recv)
    back_out[...] = back[...]

    pltpu.make_async_copy(halo, halo, hs).wait()

    pass_on.wait_send()

    @pl.when(has_two)
    def _():
        whole(got, 158, f_send)
        whole(turn, 126, c_send)

    @pl.when(is_owner & jnp.logical_not(has_two))
    def _():
        whole(got, 159, f_send)
        whole(turn, 63, c_send)

    @pl.when(jnp.logical_not(is_owner))
    def _():
        whole(got, 160, f_send)

    store.wait()


def main_call(starts, source, t):
    hbm = pl.BlockSpec(memory_space=pltpu.MemorySpace.HBM)
    slab = (FIELDS, DEPTH, NY, NX)
    vm = pltpu.VMEM
    dma = pltpu.SemaphoreType.DMA
    return pl.pallas_call(
        main_kernel,
        out_shape=(jax.ShapeDtypeStruct(slab, F32), jax.ShapeDtypeStruct((ROWS, 128), F32)),
        in_specs=[hbm] * 7,
        out_specs=(pl.BlockSpec(memory_space=pl.ANY), pl.BlockSpec(memory_space=vm)),
        scratch_shapes=[
            vm(slab, F32), vm(slab, F32),
            vm((4, 10, DEPTH, FIELDS, 8, NX), F32),
            vm((4, 2, 8, FIELDS, 8, NX), F32),
            vm(slab, F32), vm(slab, F32),
            vm((32, 128), BF16), vm((2, 512, 128), BF16), vm((2, 2, 256, 256), BF16), vm((2, 2, 256, 256), BF16), vm((8, 512), F32),
            vm((ROWS, 128), F32), vm((ROWS, 128), F32), vm((ROWS, 128), F32),
            vm((2 * SLABS * SLICES, 128), F32), vm((2 * SLABS * SLICES, 128), F32), vm((ROWS, 128), F32),
            dma((3,)), dma((2,)), dma, dma, dma((2, 8)), pltpu.SemaphoreType.REGULAR((8,)),
            dma, dma, dma, dma, dma, dma,
        ],
        compiler_params=pltpu.CompilerParams(collective_id=0, has_side_effects=True, vmem_limit_bytes=24 << 20),
        name="fine_and_scan",
    )(
        *(
            pltpu.with_memory_space_constraint(a, pltpu.MemorySpace.HBM)
            for a in (starts, source, t["cx"], t["m1"], t["m2"], t["m3"], t["powers"])
        )
    )


def last_kernel(fine, back, m4, cinv, ends, slice_norm, total_norm, held, norms, sem, norm_sem):
    rows = back[...]
    e = product(rows, m4[0], m4[1])
    copies = []
    for f in range(FIELDS):
        part = e[f * KX : (f + 1) * KX]
        high, low = split(jnp.concatenate([part[:, :256], part[:, 256:]], axis=0))
        fix = dot(jnp.concatenate([high, low, high], axis=0), cinv[...], ((0,), (0,)))
        held[f] = fine[f] + fix.reshape(DEPTH, NY, NX)
        copies.append(pltpu.make_async_copy(held.at[f], ends.at[0, f], sem))
        copies[-1].start()
    sums = jnp.sum(rows, axis=0, keepdims=True)
    cells = FIELDS * CELLS
    lane = lax.broadcasted_iota(jnp.int32, (1, 128), 1)
    one = jnp.sqrt(jnp.sum(jnp.where(lane == Q_LANE, sums, 0.0), axis=1, keepdims=True) / cells + epsilon)
    every = jnp.sqrt(jnp.sum(jnp.where(lane == T_LANE, sums, 0.0), axis=1, keepdims=True) / (cells * SLICES) + epsilon)
    norms[0, 0] = one[0, 0]
    norms[1, 0] = every[0, 0]
    norm_copies = [
        pltpu.make_async_copy(norms.at[i], out, norm_sem.at[i]) for i, out in enumerate((slice_norm, total_norm))
    ]
    for copy in norm_copies:
        copy.start()
    pltpu.make_async_copy(held, ends.at[0], sem).wait()
    for copy in norm_copies:
        copy.wait()


def last_call(fine, back, t):
    vm = pl.BlockSpec(memory_space=pltpu.VMEM)
    hbm = pl.BlockSpec(memory_space=pltpu.MemorySpace.HBM)
    return pl.pallas_call(
        last_kernel,
        out_shape=(
            jax.ShapeDtypeStruct((1, FIELDS, DEPTH, NY, NX), F32),
            jax.ShapeDtypeStruct((1,), F32),
            jax.ShapeDtypeStruct((1,), F32),
        ),
        in_specs=[vm] * 4,
        out_specs=(hbm, hbm, hbm),
        scratch_shapes=[
            pltpu.VMEM((FIELDS, DEPTH, NY, NX), F32), pltpu.SMEM((2, 1), F32),
            pltpu.SemaphoreType.DMA, pltpu.SemaphoreType.DMA((2,)),
        ],
        compiler_params=pltpu.CompilerParams(vmem_limit_bytes=8 << 20),
        name="inverse_and_add",
    )(fine, back, t["m4"], t["cinv"])


def solution(mesh):
    held = Mesh(mesh.devices.reshape(4, 8, 2, mesh.shape["space"]), (*TM, X))
    t = tables()

    def shards(starts, source):
        local = {k: jnp.asarray(v) for k, v in t.items()}
        fine, back = main_call(starts, source, local)
        return last_call(fine, back, local)

    return jax.shard_map(
        shards,
        mesh=held,
        in_specs=(P(TM, None, X, None, None), P(None, X, None, None)),
        out_specs=(P(TM, None, X, None, None), P(TM), P()),
        check_vma=False,
    )
```

```python
import functools
import math

import jax
import jax.numpy as jnp
import numpy as np
from jax import lax
from jax.experimental import pallas as pl
from jax.experimental.pallas import tpu as pltpu
from jax.sharding import Mesh
from jax.sharding import PartitionSpec as P

Y, Z, C, X = "tm_0", "tm_1", "tm_2", "space"
TM = (Y, Z, C)
MESH = pl.DeviceIdType.MESH
F32, BF16 = jnp.float32, jnp.bfloat16

FIELDS, NZ, NY, NX, SLICES = 5, 16, 64, 128, 64
SLABS, DEPTH = 4, 4
KX, KY = NX // 16, NY // 8
CELLS = NZ * NY * NX
viscosity, diffusivity, compress_rate = 0.08, 0.05, 0.25
time_step, diffusion_number = 0.5, 0.08
advect = {"x": 0.2, "y": 0.15, "z": 0.1}
epsilon = 1e-06
GREETINGS = (None, 1, 5, 10, 15, 19, 23, 27)
PASS_ON = 19
QUARTERS = 4
ROWS = FIELDS * KX
Q_LANE, T_LANE = 64, 72


def halves(table):
    table = np.asarray(table, np.float32)
    high = table.astype(BF16)
    low = (table - high.astype(np.float32)).astype(BF16)
    return high, low


def tables():
    kx, xs = np.arange(KX), np.arange(NX)
    ky = (np.arange(2 * KY) + KY) % (2 * KY) - KY
    keep = (ky != -KY).astype(np.float64)
    ax = 2 * np.pi / NX * np.outer(kx, xs)
    cx = np.concatenate([np.cos(ax), np.sin(ax)])
    weight = np.where(kx == 0, 1.0, 2.0)[:, None]
    cinv = np.concatenate([weight * np.cos(ax), weight * np.sin(ax)])
    permuted = np.arange(NY).reshape(8, 8).T.reshape(-1)
    eye = np.eye(DEPTH)

    def plane(ys):
        ay = 2 * np.pi / NY * np.outer(ys, ky)
        return np.cos(ay) * keep, np.sin(ay) * keep

    co, si = plane(permuted)
    m1 = np.zeros((2, DEPTH, NY, DEPTH, 2, 2 * KY))
    for cs, (re, im) in enumerate(((co, -si), (-si, -co))):
        m1[cs, :, :, :, 0, :] = np.einsum("ab,yk->aybk", eye, re)
        m1[cs, :, :, :, 1, :] = np.einsum("ab,yk->aybk", eye, im)
    co, si = plane(np.arange(NY))
    m4 = np.zeros((DEPTH, 2, 2 * KY, 2, DEPTH, NY))
    for cs, (re, im) in enumerate(((co, -si), (-si, -co))):
        m4[:, 0, :, cs, :, :] = np.einsum("ab,yk->akby", eye, re) / CELLS
        m4[:, 1, :, cs, :, :] = np.einsum("ab,yk->akby", eye, im) / CELLS
    m1 = m1.reshape(512, DEPTH, 2, QUARTERS, 4).transpose(0, 3, 1, 2, 4)
    m4 = m4.reshape(DEPTH, 2, QUARTERS, 4, 512).transpose(2, 0, 1, 3, 4)
    zs, kz = np.arange(NZ), np.arange(NZ)
    az = 2 * np.pi / NZ * np.outer(zs, kz)
    same = np.eye(2 * KY) * keep
    m2 = np.zeros((NZ, 2, 2 * KY, 2, NZ, 2 * KY))
    m3 = np.zeros((2, NZ, 2 * KY, NZ, 2, 2 * KY))
    for i, o, fwd in ((0, 0, np.cos(az)), (0, 1, -np.sin(az)), (1, 0, np.sin(az)), (1, 1, np.cos(az))):
        m2[:, i, :, o, :, :] = np.einsum("zq,kl->zkql", fwd, same)
        m3[o, :, :, :, i, :] = np.einsum("zq,kl->qkzl", fwd, same)
    kzs = (kz + NZ // 2) % NZ - NZ // 2
    tz, ty = 2 * np.pi / NZ * kzs, 2 * np.pi / NY * ky
    tx = 2 * np.pi / NX * kx
    real = 1.0 + diffusion_number * (
        (2 * np.cos(tz) - 2)[None, :, None] + (2 * np.cos(ty) - 2)[None, None, :] + (2 * np.cos(tx) - 2)[:, None, None]
    )
    imag = -(
        advect["z"] * np.sin(tz)[None, :, None] + advect["y"] * np.sin(ty)[None, None, :] + advect["x"] * np.sin(tx)[:, None, None]
    )
    g = ((real + 1j * imag) * keep)[:, [*range(0, NZ, 2), *range(1, NZ, 2)]].reshape(KX, NZ * 2 * KY)
    powers = np.zeros((KX, 8, 2 * NZ * 2 * KY))
    for p in range(6):
        power = g ** (2**p)
        powers[:, p] = np.concatenate([power.real, power.imag], axis=1)
    m2 = m2.reshape(SLABS, DEPTH, 2, QUARTERS, 4, 512).transpose(0, 3, 1, 2, 4, 5).reshape(SLABS, 128, 2, NZ, 2 * KY)
    m3 = m3.reshape(512, SLABS, DEPTH, 2, QUARTERS, 4).transpose(0, 1, 4, 2, 3, 5).reshape(2, NZ, 2 * KY, SLABS, 128)
    m2 = np.stack([m2[:2, :, :, odd::2].reshape(256, 256) for odd in range(2)])
    m3 = np.stack([m3[:, odd::2, :, :2].reshape(256, 256) for odd in range(2)])
    return dict(
        cx=np.concatenate(halves(cx)),
        m1=np.stack(halves(m1.reshape(512, 128))),
        m2=np.stack(halves(m2)),
        m3=np.stack(halves(m3)),
        powers=powers.astype(np.float32),
        m4=np.stack(halves(m4.reshape(128, 512))),
        cinv=np.concatenate([halves(cinv)[0], halves(cinv)[0], halves(cinv)[1]]),
    )


def split(x):
    high = x.astype(BF16)
    return high, (x - high.astype(F32)).astype(BF16)


def dot(a, b, dims=((1,), (0,))):
    return lax.dot_general(a, b, (dims, ((), ())), preferred_element_type=F32)


def product(x, high, low):
    m = x.shape[0]
    xh, xl = split(x)
    both = dot(jnp.concatenate([xh, xl], axis=0), high)
    return both[:m] + both[m:] + dot(xh, low)


def low_modes(rows, cx, m1):
    high, low = split(rows)
    a = dot(cx, high, ((1,), (1,)))
    a = a[:16] + a[16:] + dot(cx[:16], low, ((1,), (1,)))
    n = DEPTH * NY
    fields = [jnp.concatenate([a[:KX, f * n : (f + 1) * n], a[KX:, f * n : (f + 1) * n]], axis=1) for f in range(FIELDS)]
    return product(jnp.concatenate(fields, axis=0), m1[0], m1[1])


def rem(a, n):
    return lax.rem(a, jnp.int32(n))


def picked(i, values):
    out = jnp.int32(values[-1])
    for k, v in enumerate(values[:-1]):
        out = jnp.where(i == k, jnp.int32(v), out)
    return out


def main_kernel(
    starts, source, cx_h, m1_h, m2_h, m3_h, pw_h,
    fine_out, back_out,
    st, sr, q, halo, fo, fn, cx, m1, m2, m3, pw,
    spec_s, after, spec_f, got, turn, back,
    in_sem, const_sem, out_sem, hs, hr, rounds, p_send, p_recv, f_send, f_recv, c_send, c_recv,
):
    x, y, z, c = (lax.axis_index(a) for a in (X, Y, Z, C))
    at = lambda x=x, y=y, z=z, c=c: {Y: y, Z: z, C: c, X: x}
    up, down = at(x=rem(x + 1, 4)), at(x=rem(x + 3, 4))
    load_s = [
        pltpu.make_async_copy(starts.at[0, :, pl.ds(p, n)], st.at[:, pl.ds(p, n)], in_sem.at[i])
        for i, (p, n) in ((0, (0, 1)), (0, (3, 1)), (1, (1, 2)))
    ]
    load_r = pltpu.make_async_copy(source, sr, in_sem.at[2])
    for copy in load_s[:2]:
        copy.start()
    consts = [
        pltpu.make_async_copy(a, b, const_sem.at[i])
        for i, (a, b) in ((0, (cx_h, cx)), (0, (m1_h, m1)), (1, (m2_h, m2)), (1, (m3_h, m3)))
    ]
    scan_x2z = x * 2 + rem(z, 2)
    load_p = pltpu.make_async_copy(pw_h.at[scan_x2z], pw, const_sem.at[1])

    barrier = pltpu.get_barrier_semaphore()
    around = [
        up, down, at(y=rem(y + 1, 4)), at(y=rem(y + 3, 4)), at(z=rem(z + 1, 8)), at(z=rem(z + 7, 8)), at(c=1 - c),
    ]
    for device in around:
        pl.semaphore_signal(barrier, inc=1, device_id=device, device_id_type=MESH)

    def greet(k):
        for turn_by in (1, -1):
            device = (
                at(x=rem(x + turn_by + 4, 4)), at(c=1 - c),
                at(y=rem(y + turn_by + 4, 4)), at(y=rem(y + turn_by + 4, 4)),
                *[at(z=rem(z + turn_by + 8, 8))] * 4,
            )[k]
            pl.semaphore_signal(rounds.at[k], inc=1, device_id=device, device_id_type=MESH)

    load_s[0].wait()
    load_s[1].wait()
    load_s[2].start()

    def lay(planes):
        def body(r, carry):
            for plane in planes:
                for f in range(FIELDS):
                    q[0, r + 1, plane, f] = st[f, plane, pl.ds(r, 8, stride=8), :]
            return carry
        lax.fori_loop(0, 8, body, 0)

    def edges(j, last):
        for plane in range(DEPTH):
            for f in range(FIELDS):
                if last:
                    q[j, 0, plane, f] = pltpu.roll(q[j, 8, plane, f], 1, 0)
                else:
                    q[j, 9, plane, f] = pltpu.roll(q[j, 1, plane, f], 7, 0)

    def sends(j, r):
        return (
            pltpu.make_async_remote_copy(
                q.at[j, r + 1, 0], halo.at[j, 1, r], hs, hr.at[j % 2, r], device_id=down, device_id_type=MESH
            ),
            pltpu.make_async_remote_copy(
                q.at[j, r + 1, DEPTH - 1], halo.at[j, 0, r], hs, hr.at[j % 2, r], device_id=up, device_id_type=MESH
            ),
        )

    lay((0, 3))
    pl.semaphore_wait(barrier, len(around))
    greet(0)

    def first(r, carry):
        for copy in sends(0, r):
            copy.start()
        return carry
    lax.fori_loop(0, 8, first, 0)
    for copy in (*consts[:2], load_r, *consts[2:], load_p):
        copy.start()
    load_s[2].wait()
    lay((1, 2))
    edges(0, False)
    edges(0, True)

    consts[0].wait()
    consts[1].wait()
    spec_s[...] = low_modes(
        jnp.concatenate([q[0, 1:9, p, f].reshape(NY, NX) for f in range(FIELDS) for p in range(DEPTH)], axis=0), cx[...], m1
    )
    load_r.wait()

    is_owner = c == 1
    has_two = is_owner & (y == 0)
    mine = (y * 8 + z) * 2 + c

    before = rem(mine + SLICES - 1, SLICES)
    pass_on = pltpu.make_async_remote_copy(
        spec_s, after, p_send, p_recv,
        device_id=at(y=lax.div(before, jnp.int32(16)), z=rem(lax.div(before, jnp.int32(2)), 8), c=rem(before, 2)),
        device_id_type=MESH,
    )

    def spread(tz):
        slot = x * SLICES + rem(mine + 1, SLICES)
        for dx in (2, 1, 3, 0):
            tx = rem(x + dx, 4)
            kx = tx * 2 + rem(tz, 2)
            for dy in (2, 1, 3, 0, None):
                ty = jnp.int32(0) if dy is None else rem(y + dy, 4)
                row = (32 if dy is None else ty * KX) + kx
                here = spec_f.at[pl.ds(row, 1)]
                there = got.at[pl.ds(slot + (SLABS * SLICES if dy is None else 0), 1)]

                def far():
                    pltpu.make_async_remote_copy(
                        here, there, f_send, f_recv, device_id=at(tx, ty, tz, jnp.int32(1)), device_id_type=MESH
                    ).start()

                if dx or dy:
                    far()
                    continue
                own = (tz == z) & (ty == y) & is_owner
                pl.when(jnp.logical_not(own))(far)

                @pl.when(own)
                def _():
                    pltpu.make_async_copy(here, there, f_recv).start()

    def stage(j):
        def body(i, carry):
            r = rem(i + j, 8)
            pltpu.make_async_copy(halo.at[j, :, r], halo.at[j, :, r], hr.at[j % 2, r]).wait()
            for k, turn_at in enumerate(GREETINGS):
                if turn_at is None or turn_at // 8 != j:
                    continue

                @pl.when(i == turn_at % 8)
                def _():
                    pl.semaphore_wait(rounds.at[k - 1], 2)
                    greet(k)
                    if turn_at == PASS_ON:
                        pass_on.start()

            for plane in (0, 3, 1, 2):
                cur = [q[j, r + 1, plane, f] for f in range(FIELDS)]
                yp = [q[j, r + 2, plane, f] for f in range(FIELDS)]
                ym = [q[j, r, plane, f] for f in range(FIELDS)]
                zp = [(halo[j, 1, r, f] if plane == 3 else q[j, r + 1, plane + 1, f]) for f in range(FIELDS)]
                zm = [(halo[j, 0, r, f] if plane == 0 else q[j, r + 1, plane - 1, f]) for f in range(FIELDS)]

                def flux(v, axis, sign):
                    half = 0.5 * advect["xyz"[axis]] + 0.5 * v[axis]
                    a = viscosity - half if sign > 0 else viscosity + half
                    b = diffusivity - half if sign > 0 else diffusivity + half
                    out = [a * v[0], a * v[1], a * v[2], b * v[4]]
                    push = 0.5 * v[3]
                    out[axis] = out[axis] - push if sign > 0 else out[axis] + push
                    return out

                xplus = [pltpu.roll(v, NX - 1, 1) for v in flux(cur, 0, 1)]
                xminus = [pltpu.roll(v, 1, 1) for v in flux(cur, 0, -1)]
                parts = (xplus, xminus, flux(yp, 1, 1), flux(ym, 1, -1), flux(zp, 2, 1), flux(zm, 2, -1))
                diverge = (
                    (pltpu.roll(cur[0], NX - 1, 1) - pltpu.roll(cur[0], 1, 1)) + (yp[1] - ym[1]) + (zp[2] - zm[2])
                )
                src = [sr[f, plane, pl.ds(r, 8, stride=8), :] for f in range(FIELDS)]
                rates = [None] * FIELDS
                for n, f in enumerate((0, 1, 2, 4)):
                    coefficient = -6.0 * (viscosity if f < 3 else diffusivity)
                    total = coefficient * cur[f] + src[f]
                    pairs = [p[n] for p in parts]
                    rates[f] = total + ((pairs[0] + pairs[1]) + (pairs[2] + pairs[3]) + (pairs[4] + pairs[5]))
                rates[3] = src[3] - (0.5 * compress_rate) * diverge
                for f in range(FIELDS):
                    begin = q[0, r + 1, plane, f]
                    if j < 3:
                        step = time_step * (0.5 if j < 2 else 1.0)
                        q[j + 1, r + 1, plane, f] = begin + step * rates[f]
                    else:
                        two = q[2, r + 1, plane, f]
                        states = (q[1, r + 1, plane, f] + two) + (two + cur[f]) - begin
                        fo[f, plane, pl.ds(pl.multiple_of(r * 8, 8), 8), :] = (1.0 / 3.0) * states + (
                            time_step / 6.0
                        ) * rates[f]
            if j < 3:
                for copy in sends(j + 1, r):
                    copy.start()
                pl.when(r == 0)(lambda: edges(j + 1, False))
                pl.when(r == 7)(lambda: edges(j + 1, True))
            return carry
        lax.fori_loop(0, 8, body, 0)

    for j in range(4):
        stage(j)
    pl.semaphore_wait(rounds.at[7], 2)

    modes = low_modes(fo[...].reshape(FIELDS * DEPTH * NY, NX), cx[...], m1)
    pass_on.wait_recv()
    spec_f[...] = modes - after[...]

    def fine_rows(i, carry):
        spread(picked(i, (0, 1, 7, 2, 6, 3, 5, 4)))
        return carry
    lax.fori_loop(0, 8, fine_rows, 0)

    def plain(a, carry):
        for f in range(FIELDS):
            for p in range(DEPTH):
                fn[f, p, pl.ds(pl.multiple_of(a * 8, 8), 8), :] = fo[f, p, pl.ds(a, 8, stride=8), :]
        return carry
    lax.fori_loop(0, 8, plain, 0)
    store = pltpu.make_async_copy(fn, fine_out, out_sem)
    store.start()
    consts[2].wait()
    consts[3].wait()
    load_p.wait()

    def whole(ref, n, sem):
        pltpu.make_async_copy(ref.at[pl.ds(0, n)], ref.at[pl.ds(0, n)], sem).wait()

    def own(tasks):
        whole(got, tasks * SLABS * SLICES, f_recv)
        later = lax.broadcasted_iota(jnp.int32, (SLICES, 128), 0) > 0
        blocks = ([], [])
        for t in range(tasks):
            at_row = lambda s: (t * SLABS + s) * SLICES
            jumps = [jnp.where(later, got[at_row(s) : at_row(s) + SLICES], 0.0) for s in range(SLABS)]
            blocks[0].append(jnp.concatenate([jumps[0] + jumps[2], jumps[1] + jumps[3]], axis=1))
            blocks[1].append(jnp.concatenate([jumps[0] - jumps[2], jumps[1] - jumps[3]], axis=1))
        even, odd = (product(jnp.concatenate(blocks[i], axis=0), m2[0, i], m2[1, i]) for i in range(2))
        half = NZ * 2 * KY

        def times(p, re, im):
            gr, gi = pw[p : p + 1, :half], pw[p : p + 1, half:]
            return gr * re - gi * im, gr * im + gi * re

        weight = jnp.where(scan_x2z == 0, 1.0, 2.0) / CELLS
        fixes, sums = [], []
        for t in range(tasks):
            parts = [v[t * SLICES : (t + 1) * SLICES] for v in (even, odd)]
            re, im = times(0, *(jnp.concatenate([v[:, i : i + 128] for v in parts], axis=1) for i in (0, 128)))
            for p in range(6):
                zero = jnp.zeros((2**p, half), F32)
                shifted = (jnp.concatenate([zero, v[: -(2**p)]], axis=0) for v in (re, im))
                pr, pi = times(p, *shifted)
                re, im = re + pr, im + pi
            sums.append(jnp.sum(re * re + im * im, axis=1, keepdims=True) * weight)
            fixes.append([jnp.concatenate([re[:, i : i + 128], im[:, i : i + 128]], axis=1) for i in (0, 128)])
        even, odd = (product(jnp.concatenate([v[i] for v in fixes], axis=0), m3[0, i], m3[1, i]) for i in range(2))
        out = (even + odd, even - odd)
        lane = lax.broadcasted_iota(jnp.int32, (SLICES, 128), 1)
        for t in range(tasks):
            total = jnp.sum(sums[t], axis=0, keepdims=True)
            for s in range(SLABS):
                piece = out[s // 2][t * SLICES : (t + 1) * SLICES, s % 2 * 128 : s % 2 * 128 + 128]
                row = (t * SLABS + s) * SLICES
                turn[row : row + SLICES] = jnp.where(lane == T_LANE, total, jnp.where(lane == Q_LANE, sums[t], piece))

        def give(tx, carry):
            for ty in range(4):
                for dz in range(2):
                    tz = z - rem(z, 2) + dz
                    for tc in (1, 0):
                        for t in range(tasks):
                            here = turn.at[pl.ds((t * SLABS + tx) * SLICES + (ty * 8 + tz) * 2 + tc, 1)]
                            there = back.at[pl.ds((FIELDS - 1 if t else y) * KX + scan_x2z, 1)]

                            def far():
                                pltpu.make_async_remote_copy(
                                    here, there, c_send, c_recv,
                                    device_id=at(tx, jnp.int32(ty), tz, jnp.int32(tc)), device_id_type=MESH,
                                ).start()

                            if tc == 0:
                                far()
                                continue
                            mine_too = (tx == x) & (y == ty) & (tz == z)
                            pl.when(jnp.logical_not(mine_too))(far)

                            @pl.when(mine_too)
                            def _():
                                pltpu.make_async_copy(here, there, c_recv).start()
            return carry
        lax.fori_loop(0, 4, give, 0)

    pl.when(has_two)(lambda: own(2))
    pl.when(is_owner & jnp.logical_not(has_two))(lambda: own(1))

    whole(back, ROWS, c_recv)
    back_out[...] = back[...]

    pltpu.make_async_copy(halo, halo, hs).wait()

    pass_on.wait_send()

    @pl.when(has_two)
    def _():
        whole(got, 158, f_send)
        whole(turn, 126, c_send)

    @pl.when(is_owner & jnp.logical_not(has_two))
    def _():
        whole(got, 159, f_send)
        whole(turn, 63, c_send)

    @pl.when(jnp.logical_not(is_owner))
    def _():
        whole(got, 160, f_send)

    store.wait()


def main_call(starts, source, t):
    hbm = pl.BlockSpec(memory_space=pltpu.MemorySpace.HBM)
    slab = (FIELDS, DEPTH, NY, NX)
    vm = pltpu.VMEM
    dma = pltpu.SemaphoreType.DMA
    return pl.pallas_call(
        main_kernel,
        out_shape=(jax.ShapeDtypeStruct(slab, F32), jax.ShapeDtypeStruct((ROWS, 128), F32)),
        in_specs=[hbm] * 7,
        out_specs=(pl.BlockSpec(memory_space=pl.ANY), pl.BlockSpec(memory_space=vm)),
        scratch_shapes=[
            vm(slab, F32), vm(slab, F32),
            vm((4, 10, DEPTH, FIELDS, 8, NX), F32),
            vm((4, 2, 8, FIELDS, 8, NX), F32),
            vm(slab, F32), vm(slab, F32),
            vm((32, 128), BF16), vm((2, 512, 128), BF16), vm((2, 2, 256, 256), BF16), vm((2, 2, 256, 256), BF16), vm((8, 512), F32),
            vm((ROWS, 128), F32), vm((ROWS, 128), F32), vm((ROWS, 128), F32),
            vm((2 * SLABS * SLICES, 128), F32), vm((2 * SLABS * SLICES, 128), F32), vm((ROWS, 128), F32),
            dma((3,)), dma((2,)), dma, dma, dma((2, 8)), pltpu.SemaphoreType.REGULAR((8,)),
            dma, dma, dma, dma, dma, dma,
        ],
        compiler_params=pltpu.CompilerParams(collective_id=0, has_side_effects=True, vmem_limit_bytes=24 << 20),
        name="fine_and_scan",
    )(
        *(
            pltpu.with_memory_space_constraint(a, pltpu.MemorySpace.HBM)
            for a in (starts, source, t["cx"], t["m1"], t["m2"], t["m3"], t["powers"])
        )
    )


def last_kernel(fine, back, m4, cinv, ends, slice_norm, total_norm, held, norms, sem, norm_sem):
    rows = back[...]
    e = product(rows, m4[0], m4[1])
    copies = []
    for f in range(FIELDS):
        part = e[f * KX : (f + 1) * KX]
        high, low = split(jnp.concatenate([part[:, :256], part[:, 256:]], axis=0))
        fix = dot(jnp.concatenate([high, low, high], axis=0), cinv[...], ((0,), (0,)))
        held[f] = fine[f] + fix.reshape(DEPTH, NY, NX)
        copies.append(pltpu.make_async_copy(held.at[f], ends.at[0, f], sem))
        copies[-1].start()
    sums = jnp.sum(rows, axis=0, keepdims=True)
    cells = FIELDS * CELLS
    lane = lax.broadcasted_iota(jnp.int32, (1, 128), 1)
    one = jnp.sqrt(jnp.sum(jnp.where(lane == Q_LANE, sums, 0.0), axis=1, keepdims=True) / cells + epsilon)
    every = jnp.sqrt(jnp.sum(jnp.where(lane == T_LANE, sums, 0.0), axis=1, keepdims=True) / (cells * SLICES) + epsilon)
    norms[0, 0] = one[0, 0]
    norms[1, 0] = every[0, 0]
    norm_copies = [
        pltpu.make_async_copy(norms.at[i], out, norm_sem.at[i]) for i, out in enumerate((slice_norm, total_norm))
    ]
    for copy in norm_copies:
        copy.start()
    pltpu.make_async_copy(held, ends.at[0], sem).wait()
    for copy in norm_copies:
        copy.wait()


def last_call(fine, back, t):
    vm = pl.BlockSpec(memory_space=pltpu.VMEM)
    hbm = pl.BlockSpec(memory_space=pltpu.MemorySpace.HBM)
    return pl.pallas_call(
        last_kernel,
        out_shape=(
            jax.ShapeDtypeStruct((1, FIELDS, DEPTH, NY, NX), F32),
            jax.ShapeDtypeStruct((1,), F32),
            jax.ShapeDtypeStruct((1,), F32),
        ),
        in_specs=[vm] * 4,
        out_specs=(hbm, hbm, hbm),
        scratch_shapes=[
            pltpu.VMEM((FIELDS, DEPTH, NY, NX), F32), pltpu.SMEM((2, 1), F32),
            pltpu.SemaphoreType.DMA, pltpu.SemaphoreType.DMA((2,)),
        ],
        compiler_params=pltpu.CompilerParams(vmem_limit_bytes=8 << 20),
        name="inverse_and_add",
    )(fine, back, t["m4"], t["cinv"])


def solution(mesh):
    held = Mesh(mesh.devices.reshape(4, 8, 2, mesh.shape["space"]), (*TM, X))
    t = tables()

    def shards(starts, source):
        local = {k: jnp.asarray(v) for k, v in t.items()}
        fine, back = main_call(starts, source, local)
        return last_call(fine, back, local)

    return jax.shard_map(
        shards,
        mesh=held,
        in_specs=(P(TM, None, X, None, None), P(None, X, None, None)),
        out_specs=(P(TM, None, X, None, None), P(TM), P()),
        check_vma=False,
    )
```

```python
import functools
import math

import jax
import jax.numpy as jnp
import numpy as np
from jax import lax
from jax.experimental import pallas as pl
from jax.experimental.pallas import tpu as pltpu
from jax.sharding import Mesh
from jax.sharding import PartitionSpec as P

Y, Z, C, X = "tm_0", "tm_1", "tm_2", "space"
TM = (Y, Z, C)
MESH = pl.DeviceIdType.MESH
F32, BF16 = jnp.float32, jnp.bfloat16

FIELDS, NZ, NY, NX, SLICES = 5, 16, 64, 128, 64
SLABS, DEPTH = 4, 4
KX, KY = NX // 16, NY // 8
CELLS = NZ * NY * NX
viscosity, diffusivity, compress_rate = 0.08, 0.05, 0.25
time_step, diffusion_number = 0.5, 0.08
advect = {"x": 0.2, "y": 0.15, "z": 0.1}
epsilon = 1e-06
GREETINGS = (None, 1, 5, 10, 15, 19, 23, 27)
PASS_ON = 19
QUARTERS = 4
ROWS = FIELDS * KX
Q_LANE, T_LANE = 64, 72


def halves(table):
    table = np.asarray(table, np.float32)
    high = table.astype(BF16)
    low = (table - high.astype(np.float32)).astype(BF16)
    return high, low


def tables():
    kx, xs = np.arange(KX), np.arange(NX)
    ky = (np.arange(2 * KY) + KY) % (2 * KY) - KY
    keep = (ky != -KY).astype(np.float64)
    ax = 2 * np.pi / NX * np.outer(kx, xs)
    cx = np.concatenate([np.cos(ax), np.sin(ax)])
    weight = np.where(kx == 0, 1.0, 2.0)[:, None]
    cinv = np.concatenate([weight * np.cos(ax), weight * np.sin(ax)])
    permuted = np.arange(NY).reshape(8, 8).T.reshape(-1)
    eye = np.eye(DEPTH)

    def plane(ys):
        ay = 2 * np.pi / NY * np.outer(ys, ky)
        return np.cos(ay) * keep, np.sin(ay) * keep

    co, si = plane(permuted)
    m1 = np.zeros((2, DEPTH, NY, DEPTH, 2, 2 * KY))
    for cs, (re, im) in enumerate(((co, -si), (-si, -co))):
        m1[cs, :, :, :, 0, :] = np.einsum("ab,yk->aybk", eye, re)
        m1[cs, :, :, :, 1, :] = np.einsum("ab,yk->aybk", eye, im)
    co, si = plane(np.arange(NY))
    m4 = np.zeros((DEPTH, 2, 2 * KY, 2, DEPTH, NY))
    for cs, (re, im) in enumerate(((co, -si), (-si, -co))):
        m4[:, 0, :, cs, :, :] = np.einsum("ab,yk->akby", eye, re) / CELLS
        m4[:, 1, :, cs, :, :] = np.einsum("ab,yk->akby", eye, im) / CELLS
    m1 = m1.reshape(512, DEPTH, 2, QUARTERS, 4).transpose(0, 3, 1, 2, 4)
    m4 = m4.reshape(DEPTH, 2, QUARTERS, 4, 512).transpose(2, 0, 1, 3, 4)
    zs, kz = np.arange(NZ), np.arange(NZ)
    az = 2 * np.pi / NZ * np.outer(zs, kz)
    same = np.eye(2 * KY) * keep
    m2 = np.zeros((NZ, 2, 2 * KY, 2, NZ, 2 * KY))
    m3 = np.zeros((2, NZ, 2 * KY, NZ, 2, 2 * KY))
    for i, o, fwd in ((0, 0, np.cos(az)), (0, 1, -np.sin(az)), (1, 0, np.sin(az)), (1, 1, np.cos(az))):
        m2[:, i, :, o, :, :] = np.einsum("zq,kl->zkql", fwd, same)
        m3[o, :, :, :, i, :] = np.einsum("zq,kl->qkzl", fwd, same)
    kzs = (kz + NZ // 2) % NZ - NZ // 2
    tz, ty = 2 * np.pi / NZ * kzs, 2 * np.pi / NY * ky
    tx = 2 * np.pi / NX * kx
    real = 1.0 + diffusion_number * (
        (2 * np.cos(tz) - 2)[None, :, None] + (2 * np.cos(ty) - 2)[None, None, :] + (2 * np.cos(tx) - 2)[:, None, None]
    )
    imag = -(
        advect["z"] * np.sin(tz)[None, :, None] + advect["y"] * np.sin(ty)[None, None, :] + advect["x"] * np.sin(tx)[:, None, None]
    )
    g = ((real + 1j * imag) * keep)[:, [*range(0, NZ, 2), *range(1, NZ, 2)]].reshape(KX, NZ * 2 * KY)
    powers = np.zeros((KX, 8, 2 * NZ * 2 * KY))
    for p in range(6):
        power = g ** (2**p)
        powers[:, p] = np.concatenate([power.real, power.imag], axis=1)
    m2 = m2.reshape(SLABS, DEPTH, 2, QUARTERS, 4, 512).transpose(0, 3, 1, 2, 4, 5).reshape(SLABS, 128, 2, NZ, 2 * KY)
    m3 = m3.reshape(512, SLABS, DEPTH, 2, QUARTERS, 4).transpose(0, 1, 4, 2, 3, 5).reshape(2, NZ, 2 * KY, SLABS, 128)
    m2 = np.stack([m2[:2, :, :, odd::2].reshape(256, 256) for odd in range(2)])
    m3 = np.stack([m3[:, odd::2, :, :2].reshape(256, 256) for odd in range(2)])
    return dict(
        cx=np.concatenate(halves(cx)),
        m1=np.stack(halves(m1.reshape(512, 128))),
        m2=np.stack(halves(m2)),
        m3=np.stack(halves(m3)),
        powers=powers.astype(np.float32),
        m4=np.stack(halves(m4.reshape(128, 512))),
        cinv=np.concatenate([halves(cinv)[0], halves(cinv)[0], halves(cinv)[1]]),
    )


def split(x):
    high = x.astype(BF16)
    return high, (x - high.astype(F32)).astype(BF16)


def dot(a, b, dims=((1,), (0,))):
    return lax.dot_general(a, b, (dims, ((), ())), preferred_element_type=F32)


def product(x, high, low):
    m = x.shape[0]
    xh, xl = split(x)
    both = dot(jnp.concatenate([xh, xl], axis=0), high)
    return both[:m] + both[m:] + dot(xh, low)


def low_modes(field_rows, cx, m1):
    out = []
    for f in range(FIELDS):
        high, low = split(field_rows(f))
        a = dot(cx, high, ((1,), (1,)))
        a = a[:16] + a[16:] + dot(cx[:16], low, ((1,), (1,)))
        out.append(jnp.concatenate([a[:KX], a[KX:]], axis=1))
    return product(jnp.concatenate(out, axis=0), m1[0], m1[1])


def rem(a, n):
    return lax.rem(a, jnp.int32(n))


def picked(i, values):
    out = jnp.int32(values[-1])
    for k, v in enumerate(values[:-1]):
        out = jnp.where(i == k, jnp.int32(v), out)
    return out


def main_kernel(
    starts, source, cx_h, m1_h, m2_h, m3_h, pw_h,
    fine_out, back_out,
    st, sr, q, halo, fo, fn, cx, m1, m2, m3, pw,
    spec_s, after, spec_f, got, turn, back,
    in_sem, const_sem, out_sem, hs, hr, rounds, p_send, p_recv, f_send, f_recv, c_send, c_recv,
):
    x, y, z, c = (lax.axis_index(a) for a in (X, Y, Z, C))
    at = lambda x=x, y=y, z=z, c=c: {Y: y, Z: z, C: c, X: x}
    up, down = at(x=rem(x + 1, 4)), at(x=rem(x + 3, 4))
    load_s = [
        pltpu.make_async_copy(starts.at[0, :, pl.ds(p, n)], st.at[:, pl.ds(p, n)], in_sem.at[i])
        for i, (p, n) in ((0, (0, 1)), (0, (3, 1)), (1, (1, 2)))
    ]
    load_r = pltpu.make_async_copy(source, sr, in_sem.at[2])
    for copy in load_s[:2]:
        copy.start()
    consts = [
        pltpu.make_async_copy(a, b, const_sem.at[i])
        for i, (a, b) in ((0, (cx_h, cx)), (0, (m1_h, m1)), (1, (m2_h, m2)), (1, (m3_h, m3)))
    ]
    scan_x2z = x * 2 + rem(z, 2)
    load_p = pltpu.make_async_copy(pw_h.at[scan_x2z], pw, const_sem.at[1])

    barrier = pltpu.get_barrier_semaphore()
    around = [
        up, down, at(y=rem(y + 1, 4)), at(y=rem(y + 3, 4)), at(z=rem(z + 1, 8)), at(z=rem(z + 7, 8)), at(c=1 - c),
    ]
    for device in around:
        pl.semaphore_signal(barrier, inc=1, device_id=device, device_id_type=MESH)

    def greet(k):
        for turn_by in (1, -1):
            device = (
                at(x=rem(x + turn_by + 4, 4)), at(c=1 - c),
                at(y=rem(y + turn_by + 4, 4)), at(y=rem(y + turn_by + 4, 4)),
                *[at(z=rem(z + turn_by + 8, 8))] * 4,
            )[k]
            pl.semaphore_signal(rounds.at[k], inc=1, device_id=device, device_id_type=MESH)

    load_s[0].wait()
    load_s[1].wait()
    load_s[2].start()

    def lay(planes):
        def body(r, carry):
            for plane in planes:
                for f in range(FIELDS):
                    q[0, r + 1, plane, f] = st[f, plane, pl.ds(r, 8, stride=8), :]
            return carry
        lax.fori_loop(0, 8, body, 0)

    def edges(j, last):
        for plane in range(DEPTH):
            for f in range(FIELDS):
                if last:
                    q[j, 0, plane, f] = pltpu.roll(q[j, 8, plane, f], 1, 0)
                else:
                    q[j, 9, plane, f] = pltpu.roll(q[j, 1, plane, f], 7, 0)

    def sends(j, r):
        return (
            pltpu.make_async_remote_copy(
                q.at[j, r + 1, 0], halo.at[j, 1, r], hs, hr.at[j % 2, r], device_id=down, device_id_type=MESH
            ),
            pltpu.make_async_remote_copy(
                q.at[j, r + 1, DEPTH - 1], halo.at[j, 0, r], hs, hr.at[j % 2, r], device_id=up, device_id_type=MESH
            ),
        )

    lay((0, 3))
    pl.semaphore_wait(barrier, len(around))
    greet(0)

    def first(r, carry):
        for copy in sends(0, r):
            copy.start()
        return carry
    lax.fori_loop(0, 8, first, 0)
    for copy in (*consts[:2], load_r, *consts[2:], load_p):
        copy.start()
    load_s[2].wait()
    lay((1, 2))
    edges(0, False)
    edges(0, True)

    consts[0].wait()
    consts[1].wait()
    spec_s[...] = low_modes(
        lambda f: jnp.concatenate([q[0, 1:9, p, f].reshape(NY, NX) for p in range(DEPTH)], axis=0), cx[...], m1
    )
    load_r.wait()

    is_owner = c == 1
    has_two = is_owner & (y == 0)
    mine = (y * 8 + z) * 2 + c

    before = rem(mine + SLICES - 1, SLICES)
    pass_on = pltpu.make_async_remote_copy(
        spec_s, after, p_send, p_recv,
        device_id=at(y=lax.div(before, jnp.int32(16)), z=rem(lax.div(before, jnp.int32(2)), 8), c=rem(before, 2)),
        device_id_type=MESH,
    )

    def spread(tz):
        slot = x * SLICES + rem(mine + 1, SLICES)
        for dx in (2, 1, 3, 0):
            tx = rem(x + dx, 4)
            kx = tx * 2 + rem(tz, 2)
            for dy in (2, 1, 3, 0, None):
                ty = jnp.int32(0) if dy is None else rem(y + dy, 4)
                row = (32 if dy is None else ty * KX) + kx
                here = spec_f.at[pl.ds(row, 1)]
                there = got.at[pl.ds(slot + (SLABS * SLICES if dy is None else 0), 1)]

                def far():
                    pltpu.make_async_remote_copy(
                        here, there, f_send, f_recv, device_id=at(tx, ty, tz, jnp.int32(1)), device_id_type=MESH
                    ).start()

                if dx or dy:
                    far()
                    continue
                own = (tz == z) & (ty == y) & is_owner
                pl.when(jnp.logical_not(own))(far)

                @pl.when(own)
                def _():
                    pltpu.make_async_copy(here, there, f_recv).start()

    def stage(j):
        def body(i, carry):
            r = rem(i + j, 8)
            pltpu.make_async_copy(halo.at[j, :, r], halo.at[j, :, r], hr.at[j % 2, r]).wait()
            for k, turn_at in enumerate(GREETINGS):
                if turn_at is None or turn_at // 8 != j:
                    continue

                @pl.when(i == turn_at % 8)
                def _():
                    pl.semaphore_wait(rounds.at[k - 1], 2)
                    greet(k)
                    if turn_at == PASS_ON:
                        pass_on.start()

            for plane in (0, 3, 1, 2):
                cur = [q[j, r + 1, plane, f] for f in range(FIELDS)]
                yp = [q[j, r + 2, plane, f] for f in range(FIELDS)]
                ym = [q[j, r, plane, f] for f in range(FIELDS)]
                zp = [(halo[j, 1, r, f] if plane == 3 else q[j, r + 1, plane + 1, f]) for f in range(FIELDS)]
                zm = [(halo[j, 0, r, f] if plane == 0 else q[j, r + 1, plane - 1, f]) for f in range(FIELDS)]

                def flux(v, axis, sign):
                    half = 0.5 * advect["xyz"[axis]] + 0.5 * v[axis]
                    a = viscosity - half if sign > 0 else viscosity + half
                    b = diffusivity - half if sign > 0 else diffusivity + half
                    out = [a * v[0], a * v[1], a * v[2], b * v[4]]
                    push = 0.5 * v[3]
                    out[axis] = out[axis] - push if sign > 0 else out[axis] + push
                    return out

                xplus = [pltpu.roll(v, NX - 1, 1) for v in flux(cur, 0, 1)]
                xminus = [pltpu.roll(v, 1, 1) for v in flux(cur, 0, -1)]
                parts = (xplus, xminus, flux(yp, 1, 1), flux(ym, 1, -1), flux(zp, 2, 1), flux(zm, 2, -1))
                diverge = (
                    (pltpu.roll(cur[0], NX - 1, 1) - pltpu.roll(cur[0], 1, 1)) + (yp[1] - ym[1]) + (zp[2] - zm[2])
                )
                src = [sr[f, plane, pl.ds(r, 8, stride=8), :] for f in range(FIELDS)]
                rates = [None] * FIELDS
                for n, f in enumerate((0, 1, 2, 4)):
                    coefficient = -6.0 * (viscosity if f < 3 else diffusivity)
                    total = coefficient * cur[f] + src[f]
                    pairs = [p[n] for p in parts]
                    rates[f] = total + ((pairs[0] + pairs[1]) + (pairs[2] + pairs[3]) + (pairs[4] + pairs[5]))
                rates[3] = src[3] - (0.5 * compress_rate) * diverge
                for f in range(FIELDS):
                    begin = q[0, r + 1, plane, f]
                    if j < 3:
                        step = time_step * (0.5 if j < 2 else 1.0)
                        q[j + 1, r + 1, plane, f] = begin + step * rates[f]
                    else:
                        two = q[2, r + 1, plane, f]
                        states = (q[1, r + 1, plane, f] + two) + (two + cur[f]) - begin
                        fo[f, plane, pl.ds(pl.multiple_of(r * 8, 8), 8), :] = (1.0 / 3.0) * states + (
                            time_step / 6.0
                        ) * rates[f]
            if j < 3:
                for copy in sends(j + 1, r):
                    copy.start()
                pl.when(r == 0)(lambda: edges(j + 1, False))
                pl.when(r == 7)(lambda: edges(j + 1, True))
            return carry
        lax.fori_loop(0, 8, body, 0)

    for j in range(4):
        stage(j)
    pl.semaphore_wait(rounds.at[7], 2)

    modes = low_modes(lambda f: fo[f].reshape(DEPTH * NY, NX), cx[...], m1)
    pass_on.wait_recv()
    spec_f[...] = modes - after[...]

    def fine_rows(i, carry):
        spread(picked(i, (7, 2, 6, 3, 5, 4)))
        return carry
    spread(jnp.int32(0))
    spread(jnp.int32(1))
    lax.fori_loop(0, 6, fine_rows, 0)

    def plain(a, carry):
        for f in range(FIELDS):
            for p in range(DEPTH):
                fn[f, p, pl.ds(pl.multiple_of(a * 8, 8), 8), :] = fo[f, p, pl.ds(a, 8, stride=8), :]
        return carry
    lax.fori_loop(0, 8, plain, 0)
    store = pltpu.make_async_copy(fn, fine_out, out_sem)
    store.start()
    consts[2].wait()
    consts[3].wait()
    load_p.wait()

    def whole(ref, n, sem):
        pltpu.make_async_copy(ref.at[pl.ds(0, n)], ref.at[pl.ds(0, n)], sem).wait()

    def own(tasks):
        whole(got, tasks * SLABS * SLICES, f_recv)
        later = lax.broadcasted_iota(jnp.int32, (SLICES, 128), 0) > 0
        blocks = ([], [])
        for t in range(tasks):
            at_row = lambda s: (t * SLABS + s) * SLICES
            jumps = [jnp.where(later, got[at_row(s) : at_row(s) + SLICES], 0.0) for s in range(SLABS)]
            blocks[0].append(jnp.concatenate([jumps[0] + jumps[2], jumps[1] + jumps[3]], axis=1))
            blocks[1].append(jnp.concatenate([jumps[0] - jumps[2], jumps[1] - jumps[3]], axis=1))
        even, odd = (product(jnp.concatenate(blocks[i], axis=0), m2[0, i], m2[1, i]) for i in range(2))
        half = NZ * 2 * KY

        def times(p, re, im):
            gr, gi = pw[p : p + 1, :half], pw[p : p + 1, half:]
            return gr * re - gi * im, gr * im + gi * re

        weight = jnp.where(scan_x2z == 0, 1.0, 2.0) / CELLS
        fixes, sums = [], []
        for t in range(tasks):
            parts = [v[t * SLICES : (t + 1) * SLICES] for v in (even, odd)]
            re, im = times(0, *(jnp.concatenate([v[:, i : i + 128] for v in parts], axis=1) for i in (0, 128)))
            for p in range(6):
                zero = jnp.zeros((2**p, half), F32)
                shifted = (jnp.concatenate([zero, v[: -(2**p)]], axis=0) for v in (re, im))
                pr, pi = times(p, *shifted)
                re, im = re + pr, im + pi
            sums.append(jnp.sum(re * re + im * im, axis=1, keepdims=True) * weight)
            fixes.append([jnp.concatenate([re[:, i : i + 128], im[:, i : i + 128]], axis=1) for i in (0, 128)])
        even, odd = (product(jnp.concatenate([v[i] for v in fixes], axis=0), m3[0, i], m3[1, i]) for i in range(2))
        out = (even + odd, even - odd)
        lane = lax.broadcasted_iota(jnp.int32, (SLICES, 128), 1)
        for t in range(tasks):
            total = jnp.sum(sums[t], axis=0, keepdims=True)
            for s in range(SLABS):
                piece = out[s // 2][t * SLICES : (t + 1) * SLICES, s % 2 * 128 : s % 2 * 128 + 128]
                row = (t * SLABS + s) * SLICES
                turn[row : row + SLICES] = jnp.where(lane == T_LANE, total, jnp.where(lane == Q_LANE, sums[t], piece))

        def give(tx, carry):
            for ty in range(4):
                for dz in range(2):
                    tz = z - rem(z, 2) + dz
                    for tc in (1, 0):
                        for t in range(tasks):
                            here = turn.at[pl.ds((t * SLABS + tx) * SLICES + (ty * 8 + tz) * 2 + tc, 1)]
                            there = back.at[pl.ds((FIELDS - 1 if t else y) * KX + scan_x2z, 1)]

                            def far():
                                pltpu.make_async_remote_copy(
                                    here, there, c_send, c_recv,
                                    device_id=at(tx, jnp.int32(ty), tz, jnp.int32(tc)), device_id_type=MESH,
                                ).start()

                            if tc == 0:
                                far()
                                continue
                            mine_too = (tx == x) & (y == ty) & (tz == z)
                            pl.when(jnp.logical_not(mine_too))(far)

                            @pl.when(mine_too)
                            def _():
                                pltpu.make_async_copy(here, there, c_recv).start()
            return carry
        lax.fori_loop(0, 4, give, 0)

    pl.when(has_two)(lambda: own(2))
    pl.when(is_owner & jnp.logical_not(has_two))(lambda: own(1))

    whole(back, ROWS, c_recv)
    back_out[...] = back[...]

    pltpu.make_async_copy(halo, halo, hs).wait()

    pass_on.wait_send()

    @pl.when(has_two)
    def _():
        whole(got, 158, f_send)
        whole(turn, 126, c_send)

    @pl.when(is_owner & jnp.logical_not(has_two))
    def _():
        whole(got, 159, f_send)
        whole(turn, 63, c_send)

    @pl.when(jnp.logical_not(is_owner))
    def _():
        whole(got, 160, f_send)

    store.wait()


def main_call(starts, source, t):
    hbm = pl.BlockSpec(memory_space=pltpu.MemorySpace.HBM)
    slab = (FIELDS, DEPTH, NY, NX)
    vm = pltpu.VMEM
    dma = pltpu.SemaphoreType.DMA
    return pl.pallas_call(
        main_kernel,
        out_shape=(jax.ShapeDtypeStruct(slab, F32), jax.ShapeDtypeStruct((ROWS, 128), F32)),
        in_specs=[hbm] * 7,
        out_specs=(pl.BlockSpec(memory_space=pl.ANY), pl.BlockSpec(memory_space=vm)),
        scratch_shapes=[
            vm(slab, F32), vm(slab, F32),
            vm((4, 10, DEPTH, FIELDS, 8, NX), F32),
            vm((4, 2, 8, FIELDS, 8, NX), F32),
            vm(slab, F32), vm(slab, F32),
            vm((32, 128), BF16), vm((2, 512, 128), BF16), vm((2, 2, 256, 256), BF16), vm((2, 2, 256, 256), BF16), vm((8, 512), F32),
            vm((ROWS, 128), F32), vm((ROWS, 128), F32), vm((ROWS, 128), F32),
            vm((2 * SLABS * SLICES, 128), F32), vm((2 * SLABS * SLICES, 128), F32), vm((ROWS, 128), F32),
            dma((3,)), dma((2,)), dma, dma, dma((2, 8)), pltpu.SemaphoreType.REGULAR((8,)),
            dma, dma, dma, dma, dma, dma,
        ],
        compiler_params=pltpu.CompilerParams(collective_id=0, has_side_effects=True, vmem_limit_bytes=24 << 20),
        name="fine_and_scan",
    )(
        *(
            pltpu.with_memory_space_constraint(a, pltpu.MemorySpace.HBM)
            for a in (starts, source, t["cx"], t["m1"], t["m2"], t["m3"], t["powers"])
        )
    )


def last_kernel(fine, back, m4, cinv, ends, slice_norm, total_norm, held, norms, sem, norm_sem):
    rows = back[...]
    e = product(rows, m4[0], m4[1])
    copies = []
    for f in range(FIELDS):
        part = e[f * KX : (f + 1) * KX]
        high, low = split(jnp.concatenate([part[:, :256], part[:, 256:]], axis=0))
        fix = dot(jnp.concatenate([high, low, high], axis=0), cinv[...], ((0,), (0,)))
        held[f] = fine[f] + fix.reshape(DEPTH, NY, NX)
        copies.append(pltpu.make_async_copy(held.at[f], ends.at[0, f], sem))
        copies[-1].start()
    sums = jnp.sum(rows, axis=0, keepdims=True)
    cells = FIELDS * CELLS
    lane = lax.broadcasted_iota(jnp.int32, (1, 128), 1)
    one = jnp.sqrt(jnp.sum(jnp.where(lane == Q_LANE, sums, 0.0), axis=1, keepdims=True) / cells + epsilon)
    every = jnp.sqrt(jnp.sum(jnp.where(lane == T_LANE, sums, 0.0), axis=1, keepdims=True) / (cells * SLICES) + epsilon)
    norms[0, 0] = one[0, 0]
    norms[1, 0] = every[0, 0]
    norm_copies = [
        pltpu.make_async_copy(norms.at[i], out, norm_sem.at[i]) for i, out in enumerate((slice_norm, total_norm))
    ]
    for copy in norm_copies:
        copy.start()
    pltpu.make_async_copy(held, ends.at[0], sem).wait()
    for copy in norm_copies:
        copy.wait()


def last_call(fine, back, t):
    vm = pl.BlockSpec(memory_space=pltpu.VMEM)
    hbm = pl.BlockSpec(memory_space=pltpu.MemorySpace.HBM)
    return pl.pallas_call(
        last_kernel,
        out_shape=(
            jax.ShapeDtypeStruct((1, FIELDS, DEPTH, NY, NX), F32),
            jax.ShapeDtypeStruct((1,), F32),
            jax.ShapeDtypeStruct((1,), F32),
        ),
        in_specs=[vm] * 4,
        out_specs=(hbm, hbm, hbm),
        scratch_shapes=[
            pltpu.VMEM((FIELDS, DEPTH, NY, NX), F32), pltpu.SMEM((2, 1), F32),
            pltpu.SemaphoreType.DMA, pltpu.SemaphoreType.DMA((2,)),
        ],
        compiler_params=pltpu.CompilerParams(vmem_limit_bytes=8 << 20),
        name="inverse_and_add",
    )(fine, back, t["m4"], t["cinv"])


def solution(mesh):
    held = Mesh(mesh.devices.reshape(4, 8, 2, mesh.shape["space"]), (*TM, X))
    t = tables()

    def shards(starts, source):
        local = {k: jnp.asarray(v) for k, v in t.items()}
        fine, back = main_call(starts, source, local)
        return last_call(fine, back, local)

    return jax.shard_map(
        shards,
        mesh=held,
        in_specs=(P(TM, None, X, None, None), P(None, X, None, None)),
        out_specs=(P(TM, None, X, None, None), P(TM), P()),
        check_vma=False,
    )
```
